8 devices in a mesh: fsdp: 8 (over z, y, x, core).
Axes of the slice: x: 2, y: 2, z: 1, core: 2. Of those that a mesh axis runs over, the one named last changes fastest.
Arguments:
- x_in: bfloat16 [32, 512, 2048], P('fsdp')
- grad_out: bfloat16 [32, 512, 2048], P('fsdp')
- norm_attn: bfloat16 [2048], P('fsdp')
- w_query: bfloat16 [2048, 16, 128], P('fsdp')
- w_key: bfloat16 [2048, 16, 128], P('fsdp')
- w_value: bfloat16 [2048, 16, 128], P('fsdp')
- w_rel: bfloat16 [2048, 16, 128], P('fsdp')
- bias_u: bfloat16 [2048], P('fsdp')
- bias_w: bfloat16 [2048], P('fsdp')
- w_attn_out: bfloat16 [2048, 2048], P('fsdp')
- norm_mlp: bfloat16 [2048], P('fsdp')
- w_up: bfloat16 [2048, 8192], P('fsdp')
- w_down: bfloat16 [8192, 2048], P('fsdp')
Outputs:
- output 1: bfloat16 [32, 512, 2048], P('fsdp')
- output 2: bfloat16 [32, 512, 2048], P('fsdp')
- output 3: float32 [2048], P('fsdp')
- output 4: float32 [2048, 16, 128], P('fsdp')
- output 5: float32 [2048, 16, 128], P('fsdp')
- output 6: float32 [2048, 16, 128], P('fsdp')
- output 7: float32 [2048, 16, 128], P('fsdp')
- output 8: float32 [2048], P('fsdp')
- output 9: float32 [2048], P('fsdp')
- output 10: float32 [2048, 2048], P('fsdp')
- output 11: float32 [2048], P('fsdp')
- output 12: float32 [2048, 8192], P('fsdp')
- output 13: float32 [8192, 2048], P('fsdp')
All inputs are finite; a program needn't handle non-finite values.
Results may differ from the reference program's by a relative error of at most 0.02.
Values are sent between devices in bfloat16 or wider.
A program may use at most 1 GiB of HBM per device.

```python
import jax
import jax.numpy as jnp
from jax import lax

D = 2048
HEADS = 16
HEAD = 128
FF = 8192
SEQ = 512
BATCH = 32
EPS = 1e-6
MASK_VALUE = -1e30


def setup_inputs(seed: int = 0) -> dict:
    key_list = jax.random.split(jax.random.key(seed), 13)

    def normal(key_index, arr_shape, std_scale):
        return jax.random.normal(key_list[key_index], arr_shape, jnp.float32) * std_scale

    hidden = HEADS * HEAD
    return dict(
        x_in=normal(0, (BATCH, SEQ, D), 1.0).astype(jnp.bfloat16),
        grad_out=normal(1, (BATCH, SEQ, D), 1.0).astype(jnp.bfloat16),
        norm_attn=(1.0 + normal(2, (D,), 0.3)).astype(jnp.bfloat16),
        w_query=normal(3, (D, HEADS, HEAD), D ** -0.5).astype(jnp.bfloat16),
        w_key=normal(4, (D, HEADS, HEAD), D ** -0.5).astype(jnp.bfloat16),
        w_value=normal(5, (D, HEADS, HEAD), D ** -0.5).astype(jnp.bfloat16),
        w_rel=normal(6, (D, HEADS, HEAD), D ** -0.5).astype(jnp.bfloat16),
        bias_u=normal(7, (hidden,), 1.0).astype(jnp.bfloat16),
        bias_w=normal(8, (hidden,), 1.0).astype(jnp.bfloat16),
        w_attn_out=normal(9, (hidden, D), hidden ** -0.5).astype(jnp.bfloat16),
        norm_mlp=(1.0 + normal(10, (D,), 0.3)).astype(jnp.bfloat16),
        w_up=normal(11, (D, FF), D ** -0.5).astype(jnp.bfloat16),
        w_down=normal(12, (FF, D), FF ** -0.5).astype(jnp.bfloat16),
    )


def sin_table(seq_len, model_width):
    distance = (seq_len - 1 - jnp.arange(seq_len)).astype(jnp.float32)
    inv_freq = 10000.0 ** (-jnp.arange(0, model_width, 2).astype(jnp.float32) / model_width)
    angles = distance[:, None] * inv_freq[None, :]
    return jnp.concatenate([jnp.sin(angles), jnp.cos(angles)], axis=-1).astype(jnp.bfloat16)


def rms_norm(x_f32, gain_vec):
    mean_sq = jnp.mean(x_f32 * x_f32, axis=-1, keepdims=True)
    return (x_f32 * lax.rsqrt(mean_sq + EPS) * gain_vec).astype(jnp.bfloat16)


def rel_shift(scores):
    lead_dims = scores.shape[:-2]
    num_keys = scores.shape[-1]
    padded = jnp.pad(scores, [(0, 0)] * len(lead_dims) + [(0, 0), (1, 0)])
    padded = padded.reshape(lead_dims + (num_keys + 1, num_keys))
    return padded[..., 1:, :].reshape(lead_dims + (num_keys, num_keys))


def layer_forward(x_seq, params, pos_table):
    (norm_attn, w_query, w_key, w_value, w_rel, bias_u, bias_w, w_attn_out, norm_mlp, w_up, w_down) = params
    seq_len = x_seq.shape[0]
    x_f32 = x_seq.astype(jnp.float32)
    h_attn = rms_norm(x_f32, norm_attn).astype(jnp.float32)
    q_heads = jnp.einsum('sm,mhd->shd', h_attn, w_query).astype(jnp.bfloat16).astype(jnp.float32)
    k_heads = jnp.einsum('sm,mhd->shd', h_attn, w_key).astype(jnp.bfloat16).astype(jnp.float32)
    v_heads = jnp.einsum('sm,mhd->shd', h_attn, w_value).astype(jnp.bfloat16).astype(jnp.float32)
    r_heads = jnp.einsum('km,mhd->khd', pos_table.astype(jnp.float32), w_rel).astype(jnp.bfloat16).astype(jnp.float32)
    q_u = (q_heads + bias_u.reshape(HEADS, HEAD)).astype(jnp.bfloat16).astype(jnp.float32)
    q_w = (q_heads + bias_w.reshape(HEADS, HEAD)).astype(jnp.bfloat16).astype(jnp.float32)
    content = jnp.einsum('shd,thd->hst', q_u, k_heads)
    position = rel_shift(jnp.einsum('shd,khd->hsk', q_w, r_heads))
    logits = (content + position) * (HEAD ** -0.5)
    causal = jnp.arange(seq_len)[:, None] >= jnp.arange(seq_len)[None, :]
    attn_probs = jax.nn.softmax(jnp.where(causal, logits, MASK_VALUE), axis=-1).astype(jnp.bfloat16).astype(jnp.float32)
    context = jnp.einsum('hst,thd->shd', attn_probs, v_heads).astype(jnp.bfloat16).astype(jnp.float32)
    attn_delta = jnp.einsum('shd,hdm->sm', context, w_attn_out.reshape(HEADS, HEAD, D))
    x1_f32 = (x_f32 + attn_delta).astype(jnp.bfloat16).astype(jnp.float32)
    h_mlp = rms_norm(x1_f32, norm_mlp).astype(jnp.float32)
    pre_act = jnp.dot(h_mlp, w_up).astype(jnp.bfloat16).astype(jnp.float32)
    activated = jax.nn.gelu(pre_act, approximate=True).astype(jnp.bfloat16).astype(jnp.float32)
    return (x1_f32 + jnp.dot(activated, w_down)).astype(jnp.bfloat16)


def reference(x_in, grad_out, norm_attn, w_query, w_key, w_value, w_rel, bias_u, bias_w, w_attn_out, norm_mlp, w_up, w_down):
    params = tuple(weight.astype(jnp.float32) for weight in (norm_attn, w_query, w_key, w_value, w_rel, bias_u, bias_w, w_attn_out, norm_mlp, w_up, w_down))
    pos_table = sin_table(SEQ, D)

    def scan_step(grad_sum, seq_pair):
        x_seq, dy_seq = seq_pair
        y_seq, pullback = jax.vjp(lambda x_part, p_part: layer_forward(x_part, p_part, pos_table), x_seq, params)
        dx_seq, grad_params = pullback(dy_seq)
        return jax.tree.map(jnp.add, grad_sum, grad_params), (y_seq, dx_seq)

    zero_grads = jax.tree.map(jnp.zeros_like, params)
    grad_sum, (y_out, grad_x) = lax.scan(scan_step, zero_grads, (x_in, grad_out))
    grad_list = [grad_total / BATCH for grad_total in grad_sum]
    return (y_out, grad_x, grad_list[0], grad_list[1], grad_list[2], grad_list[3], grad_list[4], grad_list[5], grad_list[6], grad_list[7], grad_list[8], grad_list[9], grad_list[10])
```

```python
import functools

import jax
import jax.numpy as jnp
from jax import lax
from jax.experimental import pallas as pl
from jax.experimental.pallas import tpu as pltpu
from jax.sharding import PartitionSpec as P


EPS = 1e-6
MASK_VALUE = -1e30
BLK = 128
F32 = jnp.float32
BF16 = jnp.bfloat16


def sin_table(seq_len, model_width):
    distance = (seq_len - 1 - jnp.arange(seq_len)).astype(F32)
    inv_freq = 10000.0 ** (-jnp.arange(0, model_width, 2).astype(F32) / model_width)
    angles = distance[:, None] * inv_freq[None, :]
    return jnp.concatenate([jnp.sin(angles), jnp.cos(angles)], axis=-1).astype(BF16)


def rms_norm(x_f32, gain_vec):
    mean_sq = jnp.mean(x_f32 * x_f32, axis=-1, keepdims=True)
    return (x_f32 * lax.rsqrt(mean_sq + EPS) * gain_vec).astype(BF16)


def gelu_tanh(pre_f32):
    return jax.nn.gelu(pre_f32, approximate=True)


def dot_nn(a, b):
    return lax.dot_general(a, b, (((1,), (0,)), ((), ())), preferred_element_type=F32)


def dot_nt(a, b):
    return lax.dot_general(a, b, (((1,), (1,)), ((), ())), preferred_element_type=F32)


def dot_tn(a, b):
    return lax.dot_general(a, b, (((0,), (0,)), ((), ())), preferred_element_type=F32)


def after(value, *earlier):
    return lax.optimization_barrier((value, *earlier))[0]


def tril_mask():
    return lax.broadcasted_iota(jnp.int32, (BLK, BLK), 0) >= lax.broadcasted_iota(jnp.int32, (BLK, BLK), 1)


def shear(x):
    return pltpu.roll(x, 1, axis=1, stride=1, stride_axis=0)


def block_probs(q_u, q_w, keys, rel, block, seq_len, head_dim, tril):
    top = (block + 1) * BLK
    content = dot_nt(q_u, keys[:top])
    table = dot_nt(q_w, rel[seq_len - top:])
    turned = [shear(table[:, c * BLK:(c + 1) * BLK]) for c in range(block + 1)]
    scale = head_dim ** -0.5
    parts = []
    for c in range(block + 1):
        part = content[:, c * BLK:(c + 1) * BLK]
        if c < block:
            part = (part + jnp.where(tril, turned[c], turned[c + 1])) * scale
        else:
            part = jnp.where(tril, (part + turned[c]) * scale, MASK_VALUE)
        parts.append(part)
    logits = jnp.concatenate(parts, axis=1) if block else parts[0]
    grown = jnp.exp(logits - jnp.max(logits, axis=1, keepdims=True))
    return grown * (1.0 / jnp.sum(grown, axis=1, keepdims=True))


def attn_fwd_kernel(q_ref, k_ref, v_ref, r_ref, u_ref, w_ref, c_ref, *, heads, head_dim):
    seq_len = q_ref.shape[1]
    tril = tril_mask()
    for n in range(heads):
        cols = slice(n * head_dim, (n + 1) * head_dim)
        q_f32 = q_ref[0, :, cols].astype(F32)
        q_u = (q_f32 + u_ref[0, :, cols]).astype(BF16)
        q_w = (q_f32 + w_ref[0, :, cols]).astype(BF16)
        keys, vals, rel = k_ref[0, :, cols], v_ref[0, :, cols], r_ref[0, :, cols]
        for block in range(seq_len // BLK):
            rows = slice(block * BLK, (block + 1) * BLK)
            probs = block_probs(q_u[rows], q_w[rows], keys, rel, block, seq_len, head_dim, tril)
            c_ref[0, rows, cols] = dot_nn(probs.astype(BF16), vals[:(block + 1) * BLK]).astype(BF16)


def attn_bwd_kernel(q_ref, k_ref, v_ref, r_ref, u_ref, w_ref, dc_ref,
                    dq_ref, dk_ref, dv_ref, dr_ref, du_ref, dw_ref, dk_acc, dv_acc, *, heads, head_dim):
    seq_len = q_ref.shape[1]
    tril = tril_mask()
    flip = (lax.broadcasted_iota(jnp.int32, (BLK, BLK), 0) + lax.broadcasted_iota(jnp.int32, (BLK, BLK), 1)
            == BLK - 1).astype(F32).astype(BF16)
    scale = head_dim ** -0.5

    @pl.when(pl.program_id(1) == 0)
    def _():
        dr_ref[...] = jnp.zeros_like(dr_ref)
        du_ref[...] = jnp.zeros_like(du_ref)
        dw_ref[...] = jnp.zeros_like(dw_ref)

    for n in range(heads):
        cols = slice(n * head_dim, (n + 1) * head_dim)
        q_f32 = q_ref[0, :, cols].astype(F32)
        q_u = (q_f32 + u_ref[0, :, cols]).astype(BF16)
        q_w = (q_f32 + w_ref[0, :, cols]).astype(BF16)
        keys, vals, rel = k_ref[0, :, cols], v_ref[0, :, cols], r_ref[0, :, cols]
        d_ctx = dc_ref[0, :, cols]
        rel_back = jnp.concatenate(
            [dot_nn(flip, rel[c * BLK:(c + 1) * BLK]).astype(BF16) for c in range(seq_len // BLK)], axis=0)
        dk_acc[...] = jnp.zeros_like(dk_acc)
        dv_acc[...] = jnp.zeros_like(dv_acc)
        for block in range(seq_len // BLK):
            top = (block + 1) * BLK
            rows = slice(block * BLK, top)
            probs = block_probs(q_u[rows], q_w[rows], keys, rel, block, seq_len, head_dim, tril)
            d_probs = dot_nt(d_ctx[rows], vals[:top]).astype(BF16).astype(F32)
            inner = jnp.sum(probs * d_probs, axis=1, keepdims=True)
            d_logits = (probs * (d_probs - inner) * scale).astype(BF16)
            dv_acc[:top] += dot_tn(probs.astype(BF16), d_ctx[rows])
            dk_acc[:top] += dot_tn(d_logits, q_u[rows])
            d_qu = dot_nn(d_logits, keys[:top]).astype(BF16).astype(F32)
            parts = []
            for c in range(block + 1):
                turned = shear(dot_nn(d_logits[:, c * BLK:(c + 1) * BLK], flip))
                parts.append(jnp.where(tril, turned, before if c else 0.0).astype(BF16))
                before = turned
            d_table = jnp.concatenate(parts, axis=1) if block else parts[0]
            d_qw = dot_nn(d_table, rel_back[seq_len - top:]).astype(BF16).astype(F32)
            dr_ref[0, seq_len - top:, cols] += dot_tn(d_table, q_w[rows])
            dq_ref[0, rows, cols] = (d_qu + d_qw).astype(BF16)
            du_ref[0, :, cols] += jnp.sum(d_qu.reshape(BLK // 8, 8, head_dim), axis=0)
            dw_ref[0, :, cols] += jnp.sum(d_qw.reshape(BLK // 8, 8, head_dim), axis=0)
        dk_ref[0, :, cols] = dk_acc[...].astype(BF16)
        dv_ref[0, :, cols] = dv_acc[...].astype(BF16)


def attn_specs(seq_len, width, groups):
    span = width // groups
    act = pl.BlockSpec((1, seq_len, span), lambda g, b: (b, 0, g))
    rel = pl.BlockSpec((1, seq_len, span), lambda g, b: (g, 0, 0))
    vec = pl.BlockSpec((1, 1, span), lambda g, b: (g, 0, 0))
    return span, act, rel, vec


def attn_fwd(q, k, v, rel, bias_u, bias_w, head_dim):
    batch, seq_len, width = q.shape
    groups = rel.shape[0]
    span, act, rspec, vec = attn_specs(seq_len, width, groups)
    work = batch * (width // head_dim) * seq_len * seq_len * head_dim
    return pl.pallas_call(
        functools.partial(attn_fwd_kernel, heads=span // head_dim, head_dim=head_dim),
        grid=(groups, batch),
        in_specs=[act, act, act, rspec, vec, vec],
        out_specs=act,
        out_shape=jax.ShapeDtypeStruct(q.shape, BF16),
        compiler_params=pltpu.CompilerParams(dimension_semantics=("arbitrary", "arbitrary")),
        cost_estimate=pl.CostEstimate(flops=8 * work, bytes_accessed=8 * batch * seq_len * width, transcendentals=0),
        name="attn_fwd",
    )(q, k, v, rel, bias_u, bias_w)


def attn_bwd(q, k, v, rel, bias_u, bias_w, d_ctx, head_dim):
    batch, seq_len, width = q.shape
    groups = rel.shape[0]
    span, act, rspec, vec = attn_specs(seq_len, width, groups)
    vec8 = pl.BlockSpec((1, 8, span), lambda g, b: (g, 0, 0))
    work = batch * (width // head_dim) * seq_len * seq_len * head_dim
    flat = jax.ShapeDtypeStruct(q.shape, BF16)
    small = jax.ShapeDtypeStruct((groups, 8, span), F32)
    return pl.pallas_call(
        functools.partial(attn_bwd_kernel, heads=span // head_dim, head_dim=head_dim),
        grid=(groups, batch),
        in_specs=[act, act, act, rspec, vec, vec, act],
        out_specs=[act, act, act, rspec, vec8, vec8],
        out_shape=[flat, flat, flat, jax.ShapeDtypeStruct(rel.shape, F32), small, small],
        scratch_shapes=[pltpu.VMEM((seq_len, head_dim), F32), pltpu.VMEM((seq_len, head_dim), F32)],
        compiler_params=pltpu.CompilerParams(dimension_semantics=("arbitrary", "arbitrary")),
        cost_estimate=pl.CostEstimate(flops=20 * work, bytes_accessed=14 * batch * seq_len * width, transcendentals=0),
        name="attn_bwd",
    )(q, k, v, rel, bias_u, bias_w, d_ctx)


def solution(mesh):
    axis_name = mesh.axis_names[0]
    group_size = mesh.shape[axis_name]
    chips = group_size // 2
    pairs = [(d, d ^ 1) for d in range(group_size)]
    same_core = [[2 * c + core for c in range(chips)] for core in range(2)]

    def gather(local_shard):
        return lax.all_gather(local_shard, axis_name, axis=0, tiled=True)

    def local_step(x_in, grad_out, norm_attn, w_query, w_key, w_value, w_rel, bias_u, bias_w, w_attn_out, norm_mlp, w_up, w_down):
        batch_local, seq_len, width = x_in.shape
        num_heads, head_dim = w_query.shape[1], w_query.shape[2]
        hidden = num_heads * head_dim
        tokens = batch_local * seq_len
        span = hidden // group_size
        scale = 1.0 / (batch_local * group_size)
        me = lax.axis_index(axis_name)
        core = lax.rem(me, 2)

        def shares(acts, kind, half, halves):
            rows = acts.shape[1] // group_size
            part = rows // halves
            return jnp.concatenate(
                [lax.dynamic_slice(acts, (0, (2 * c + kind) * rows + half * part), (tokens, part)) for c in range(chips)],
                axis=1)

        def theirs(acts, cots, half=0, halves=1):
            mine = dot_tn(shares(acts, 1 - core, half, halves), cots)
            return mine, lax.ppermute(mine, axis_name, pairs)

        def ours(acts, cots, received, half=0, halves=1):
            return (dot_tn(shares(acts, core, half, halves), cots) + received) * scale

        def spread(summed):
            return lax.psum_scatter(summed, axis_name, scatter_dimension=0, axis_index_groups=same_core, tiled=True)

        x_f32 = x_in.reshape(tokens, width).astype(F32)
        dy = grad_out.reshape(tokens, width)
        vecs = lax.all_gather(jnp.stack([norm_attn, bias_u, bias_w, norm_mlp]), axis_name, axis=0)
        gain_attn = vecs[:, 0].reshape(width).astype(F32)
        u_full = vecs[:, 1:2].astype(F32)
        w_full = vecs[:, 2:3].astype(F32)
        gain_mlp = vecs[:, 3].reshape(width).astype(F32)

        query_full = gather(w_query.reshape(-1, hidden))
        key_full = gather(w_key.reshape(-1, hidden))
        value_full = gather(w_value.reshape(-1, hidden))
        out_full = gather(w_attn_out)
        up_full = gather(w_up)
        down_full = gather(w_down)

        pos_table = sin_table(seq_len, width)
        rel_cols = lax.all_to_all(w_rel.reshape(-1, hidden), axis_name, split_axis=1, concat_axis=0, tiled=True)
        rel_heads = lax.all_gather(dot_nn(pos_table, rel_cols).astype(BF16), axis_name, axis=0)

        h_attn = rms_norm(x_f32, gain_attn)
        shape3 = (batch_local, seq_len, hidden)
        q = dot_nn(h_attn, query_full).astype(BF16)
        k = dot_nn(h_attn, key_full).astype(BF16)
        v = dot_nn(h_attn, value_full).astype(BF16)
        q3, k3, v3 = q.reshape(shape3), k.reshape(shape3), v.reshape(shape3)
        context = attn_fwd(q3, k3, v3, rel_heads, u_full, w_full, head_dim).reshape(tokens, hidden)
        x1_f32 = (x_f32 + dot_nn(context, out_full)).astype(BF16).astype(F32)
        h_mlp = rms_norm(x1_f32, gain_mlp)
        pre_act = dot_nn(h_mlp, up_full).astype(BF16)
        gelu_out, gelu_pull = jax.vjp(gelu_tanh, pre_act.astype(F32))
        activated = gelu_out.astype(BF16)

        sent0, got0 = theirs(activated, dy, 0, 2)
        sent1, got1 = theirs(activated, dy, 1, 2)
        dy_own = after(dy, sent1)
        down0 = ours(activated, dy_own, got0, 0, 2)
        down1 = ours(activated, after(dy_own, down0), got1, 1, 2)
        grad_down = jnp.concatenate([spread(down0), spread(down1)], axis=0)

        d_act = dot_nt(after(dy, down1), down_full).astype(BF16)
        d_pre = gelu_pull(d_act.astype(F32))[0].astype(BF16)
        sent0, got0 = theirs(h_mlp, d_pre, 0, 2)
        sent1, got1 = theirs(h_mlp, d_pre, 1, 2)
        d_pre_own = after(d_pre, sent1)
        up0 = ours(h_mlp, d_pre_own, got0, 0, 2)
        up1 = ours(h_mlp, after(d_pre_own, up0), got1, 1, 2)
        grad_up = jnp.concatenate([spread(up0), spread(up1)], axis=0)

        d_h_mlp = dot_nt(after(d_pre, up1), up_full).astype(BF16)
        d_x1_norm, grad_norm_mlp = jax.vjp(rms_norm, x1_f32, gain_mlp)[1](d_h_mlp)
        d_x1 = (dy.astype(F32) + d_x1_norm).astype(BF16)
        d_context = dot_nt(d_x1, out_full).astype(BF16)
        d_q, d_k, d_v, d_rel, d_u, d_w = attn_bwd(
            q3, k3, v3, rel_heads, u_full, w_full, d_context.reshape(shape3), head_dim)
        d_q, d_k, d_v = (z.reshape(tokens, hidden) for z in (d_q, d_k, d_v))
        d_rel_own = lax.psum_scatter(d_rel, axis_name, scatter_dimension=0, tiled=True)[0]

        sent_q, got_q = theirs(h_attn, d_q)
        sent_k, got_k = theirs(h_attn, after(d_k, sent_q))
        sum_q = ours(h_attn, after(d_q, sent_k), got_q)
        sent_v, got_v = theirs(h_attn, after(d_v, sum_q))
        sum_k = ours(h_attn, after(d_k, sent_v), got_k)
        sent_o, got_o = theirs(context, after(d_x1, sum_k))
        sum_v = ours(h_attn, after(d_v, sent_o), got_v)
        grad_query, grad_key, grad_value = spread(sum_q), spread(sum_k), spread(sum_v)

        y_out = (x1_f32 + dot_nn(after(activated, sum_v), down_full)).astype(BF16)

        d_rel_own = after(d_rel_own, y_out)
        d_rel_own = jnp.flip(d_rel_own.reshape(seq_len // BLK, BLK, span), axis=1).reshape(seq_len, span).astype(BF16)
        d_rel_all = lax.all_gather(d_rel_own, axis_name, axis=0)
        table_own = lax.dynamic_slice(pos_table, (0, me * (width // group_size)), (seq_len, width // group_size))
        grad_rel = dot_tn(table_own, jnp.swapaxes(d_rel_all, 0, 1).reshape(seq_len, hidden)) * scale

        sum_o = ours(context, after(d_x1, d_rel_own), got_o)
        grad_attn_out = spread(sum_o)

        d_q_h, d_k_h, d_v_h = (after(z, sum_o) for z in (d_q, d_k, d_v))
        d_h_attn = (dot_nt(d_q_h, query_full) + dot_nt(d_k_h, key_full) + dot_nt(d_v_h, value_full)).astype(BF16)
        d_x_norm, grad_norm_attn = jax.vjp(rms_norm, x_f32, gain_attn)[1](d_h_attn)
        grad_x = (d_x1.astype(F32) + d_x_norm).astype(BF16)

        small = jnp.stack([grad_norm_attn.reshape(group_size, span), jnp.sum(d_u, axis=1), jnp.sum(d_w, axis=1),
                           grad_norm_mlp.reshape(group_size, span)], axis=1)
        small = lax.psum_scatter(small * scale, axis_name, scatter_dimension=0, tiled=True)[0]

        heads3 = (-1, num_heads, head_dim)
        return (y_out.reshape(x_in.shape), grad_x.reshape(x_in.shape), small[0], grad_query.reshape(heads3),
                grad_key.reshape(heads3), grad_value.reshape(heads3), grad_rel.reshape(heads3), small[1], small[2],
                grad_attn_out, small[3], grad_up, grad_down)

    sharded = P(axis_name)
    return jax.shard_map(local_step, mesh=mesh, in_specs=(sharded,) * 13, out_specs=(sharded,) * 13, check_vma=False)
```

```python
import functools

import jax
import jax.numpy as jnp
from jax import lax
from jax.experimental import pallas as pl
from jax.experimental.layout import Layout, with_layout_constraint
from jax.experimental.pallas import tpu as pltpu
from jax.sharding import PartitionSpec as P


EPS = 1e-6
MASK_VALUE = -1e30
BLK = 128
SUB = 64
SEQ = 512
F32 = jnp.float32
BF16 = jnp.bfloat16


def sin_table(seq_len, model_width):
    distance = (seq_len - 1 - jnp.arange(seq_len)).astype(F32)
    inv_freq = 10000.0 ** (-jnp.arange(0, model_width, 2).astype(F32) / model_width)
    angles = distance[:, None] * inv_freq[None, :]
    return jnp.concatenate([jnp.sin(angles), jnp.cos(angles)], axis=-1).astype(BF16)


def rms_norm(x_f32, gain_vec):
    mean_sq = jnp.mean(x_f32 * x_f32, axis=-1, keepdims=True)
    return (x_f32 * lax.rsqrt(mean_sq + EPS) * gain_vec).astype(BF16)


def gelu_tanh(pre_f32):
    return jax.nn.gelu(pre_f32, approximate=True)


def dot_nn(a, b):
    return lax.dot_general(a, b, (((1,), (0,)), ((), ())), preferred_element_type=F32)


def dot_nt(a, b):
    return lax.dot_general(a, b, (((1,), (1,)), ((), ())), preferred_element_type=F32)


def dot_tn(a, b):
    return lax.dot_general(a, b, (((0,), (0,)), ((), ())), preferred_element_type=F32)


def after(value, *earlier):
    return lax.optimization_barrier((value, *earlier))[0]


def tril_mask(first):
    shape = (SUB, BLK)
    return lax.broadcasted_iota(jnp.int32, shape, 0) + first >= lax.broadcasted_iota(jnp.int32, shape, 1)


def shear(x, first):
    return pltpu.roll(x, 1 + first, axis=1, stride=1, stride_axis=0)


def halves_of(seq_len):
    half = seq_len // 2
    return [(slice(h * half, (h + 1) * half), (h + 1) * half) for h in range(2)]


def fill_scores(q_u, q_w, keys, rel, s_ref, t_ref):
    seq_len = q_u.shape[0]
    for rows, top in halves_of(seq_len):
        s_ref[rows, :top] = dot_nt(q_u[rows], keys[:top])
        t_ref[rows, :top] = dot_nt(q_w[rows], rel[seq_len - top:])


def row_pieces(seq_len):
    return [(slice(at, at + SUB), at // BLK, at % BLK) for at in range(0, seq_len, SUB)]


def piece_probs(s_ref, t_ref, piece, head_dim):
    rows, block, first = piece
    tril = tril_mask(first)
    skip = 1 - block % 2
    scale = head_dim ** -0.5
    turned = [shear(t_ref[rows, (skip + c) * BLK:(skip + c + 1) * BLK], first) for c in range(block + 1)]
    parts = []
    for c in range(block + 1):
        part = s_ref[rows, c * BLK:(c + 1) * BLK]
        if c < block:
            part = (part + jnp.where(tril, turned[c], turned[c + 1])) * scale
        else:
            part = jnp.where(tril, (part + turned[c]) * scale, MASK_VALUE)
        parts.append(part)
    logits = jnp.concatenate(parts, axis=1) if block else parts[0]
    grown = jnp.exp(logits - jnp.max(logits, axis=1, keepdims=True))
    return grown * (1.0 / jnp.sum(grown, axis=1, keepdims=True))


def put_piece(ref, piece, value, front):
    rows, block, _ = piece
    width = (block + 1) * BLK
    skip = BLK if front and block % 2 == 0 else 0
    ref[rows, skip:skip + width] = value
    if block % 2 == 0:
        rest = 0 if front else width
        ref[rows, rest:rest + BLK] = jnp.zeros((SUB, BLK), ref.dtype)


def unpack_rel(r_ref):
    width = r_ref.shape[1] * r_ref.shape[2] // SEQ
    return jnp.concatenate([r_ref[0, :, at:at + width] for at in range(0, r_ref.shape[2], width)], axis=0)


def attn_fwd_kernel(qkv_ref, r_ref, u_ref, w_ref, c_ref, s_all, t_all, p_all, *, heads, head_dim):
    seq_len = qkv_ref.shape[1]
    q_ref, k_ref, v_ref = (qkv_ref.at[:, :, part * heads * head_dim:(part + 1) * heads * head_dim] for part in range(3))
    rel_pair = unpack_rel(r_ref)
    all_cols = [slice(n * head_dim, (n + 1) * head_dim) for n in range(heads)]
    for n, cols in enumerate(all_cols):
        q_f32 = q_ref[0, :, cols].astype(F32)
        q_u = (q_f32 + u_ref[0, :, cols]).astype(BF16)
        q_w = (q_f32 + w_ref[0, :, cols]).astype(BF16)
        fill_scores(q_u, q_w, k_ref[0, :, cols], rel_pair[:, cols], s_all.at[n], t_all.at[n])
    for piece in row_pieces(seq_len):
        for n in range(heads):
            put_piece(p_all.at[n], piece, piece_probs(s_all.at[n], t_all.at[n], piece, head_dim).astype(BF16), False)
    for n, cols in enumerate(all_cols):
        for rows, top in halves_of(seq_len):
            c_ref[0, rows, cols] = dot_nn(p_all[n, rows, :top], v_ref[0, :top, cols]).astype(BF16)


def attn_bwd_kernel(qkv_ref, r_ref, u_ref, w_ref, dc_ref, dqkv_ref, dr_ref, du_ref, dw_ref,
                    s_all, t_all, dp_all, p_all, ds_all, dt_all, qu_all, qw_all, rb_all, *, heads, head_dim):
    seq_len = qkv_ref.shape[1]
    parts = [slice(part * heads * head_dim, (part + 1) * heads * head_dim) for part in range(3)]
    q_ref, k_ref, v_ref = (qkv_ref.at[:, :, part] for part in parts)
    dq_ref, dk_ref, dv_ref = (dqkv_ref.at[:, :, part] for part in parts)
    rel_pair = unpack_rel(r_ref)
    blocks = seq_len // BLK
    flip = (lax.broadcasted_iota(jnp.int32, (BLK, BLK), 0) + lax.broadcasted_iota(jnp.int32, (BLK, BLK), 1)
            == BLK - 1).astype(F32).astype(BF16)
    scale = head_dim ** -0.5
    all_cols = [slice(n * head_dim, (n + 1) * head_dim) for n in range(heads)]

    @pl.when(pl.program_id(1) == 0)
    def _():
        dr_ref[...] = jnp.zeros_like(dr_ref)
        du_ref[...] = jnp.zeros_like(du_ref)
        dw_ref[...] = jnp.zeros_like(dw_ref)

    for n, cols in enumerate(all_cols):
        q_f32 = q_ref[0, :, cols].astype(F32)
        qu_all[n] = (q_f32 + u_ref[0, :, cols]).astype(BF16)
        qw_all[n] = (q_f32 + w_ref[0, :, cols]).astype(BF16)
        rel = rel_pair[:, cols]
        fill_scores(qu_all[n], qw_all[n], k_ref[0, :, cols], rel, s_all.at[n], t_all.at[n])
        for rows, top in halves_of(seq_len):
            dp_all[n, rows, :top] = dot_nt(dc_ref[0, rows, cols], v_ref[0, :top, cols]).astype(BF16)
        for c in range(blocks):
            rb_all[n, c * BLK:(c + 1) * BLK] = dot_nn(flip, rel[c * BLK:(c + 1) * BLK]).astype(BF16)
    for piece in row_pieces(seq_len):
        for n in range(heads):
            probs = piece_probs(s_all.at[n], t_all.at[n], piece, head_dim)
            d_probs = dp_all[n, piece[0], :(piece[1] + 1) * BLK].astype(F32)
            inner = jnp.sum(probs * d_probs, axis=1, keepdims=True)
            put_piece(p_all.at[n], piece, probs.astype(BF16), False)
            put_piece(ds_all.at[n], piece, (probs * (d_probs - inner) * scale).astype(BF16), False)
    for n in range(heads):
        for rows, top in halves_of(seq_len):
            for c in range(top // BLK):
                t_all[n, rows, c * BLK:(c + 1) * BLK] = dot_nn(ds_all[n, rows, c * BLK:(c + 1) * BLK], flip)
    for piece in row_pieces(seq_len):
        rows, block, first = piece
        tril = tril_mask(first)
        for n in range(heads):
            turned = [shear(t_all[n, rows, c * BLK:(c + 1) * BLK], first) for c in range(block + 1)]
            parts = [jnp.where(tril, turned[c], turned[c - 1] if c else 0.0).astype(BF16) for c in range(block + 1)]
            put_piece(dt_all.at[n], piece, jnp.concatenate(parts, axis=1) if block else parts[0], True)
    (low, near), (high, far) = halves_of(seq_len)
    for n, cols in enumerate(all_cols):
        for rows, top in halves_of(seq_len):
            d_qu = dot_nn(ds_all[n, rows, :top], k_ref[0, :top, cols]).astype(BF16).astype(F32)
            d_qw = dot_nn(dt_all[n, rows, :top], rb_all[n, seq_len - top:]).astype(BF16).astype(F32)
            dq_ref[0, rows, cols] = (d_qu + d_qw).astype(BF16)
            du_ref[0, :, cols] += jnp.sum(d_qu.reshape(-1, 8, head_dim), axis=0)
            dw_ref[0, :, cols] += jnp.sum(d_qw.reshape(-1, 8, head_dim), axis=0)
        for out_ref, left, right in ((dk_ref, ds_all.at[n], qu_all[n]), (dv_ref, p_all.at[n], dc_ref[0, :, cols])):
            whole = dot_tn(left[high, :], right[high])
            out_ref[0, :near, cols] = (whole[:near] + dot_tn(left[low, :near], right[low])).astype(BF16)
            out_ref[0, near:, cols] = whole[near:].astype(BF16)
        dr_ref[0, :, cols] += dot_tn(dt_all[n, high, :], qw_all[n, high])
        dr_ref[0, near:, cols] += dot_tn(dt_all[n, low, :near], qw_all[n, low])


def attn_args(qkv, rel, bias_u, head_dim, first):
    _, seq_len, width = qkv.shape
    groups, _, span = bias_u.shape
    lines = seq_len * span // rel.shape[2]
    at = rel.shape[1] // lines - 1
    specs = [
        pl.BlockSpec((1, seq_len, width // groups), lambda g, b: (b, 0, g + first)),
        pl.BlockSpec((1, lines, rel.shape[2]), lambda g, b: (g + first, at, 0)),
        pl.BlockSpec((1, 1, span), lambda g, b: (g + first, 0, 0)),
        pl.BlockSpec((1, 1, span), lambda g, b: (g + first, 0, 0)),
    ]
    heads = span // head_dim

    def square(*dtypes):
        return [pltpu.VMEM((heads, seq_len, seq_len), dtype) for dtype in dtypes]

    return specs, square, heads, span


def attn_fwd(qkv, rel, bias_u, bias_w, head_dim):
    batch, seq_len, width = qkv.shape
    groups = bias_u.shape[0]
    specs, square, heads, span = attn_args(qkv, rel, bias_u, head_dim, 0)
    work = batch * groups * heads * seq_len * seq_len * head_dim
    return pl.pallas_call(
        functools.partial(attn_fwd_kernel, heads=heads, head_dim=head_dim),
        grid=(groups, batch),
        in_specs=specs,
        out_specs=pl.BlockSpec((1, seq_len, span), lambda g, b: (b, 0, g)),
        out_shape=jax.ShapeDtypeStruct((batch, seq_len, groups * span), BF16),
        scratch_shapes=square(F32, F32, BF16),
        compiler_params=pltpu.CompilerParams(
            dimension_semantics=("arbitrary", "arbitrary")),
        cost_estimate=pl.CostEstimate(flops=8 * work, bytes_accessed=8 * batch * seq_len * width // 3, transcendentals=0),
        name="attn_fwd",
    )(qkv, rel, bias_u, bias_w)


def attn_bwd(qkv, rel, bias_u, bias_w, d_ctx, head_dim, first, count):
    batch, seq_len, _ = qkv.shape
    specs, square, heads, span = attn_args(qkv, rel, bias_u, head_dim, first)
    work = batch * count * heads * seq_len * seq_len * head_dim
    small = jax.ShapeDtypeStruct((count, 8, span), F32)
    vec8 = pl.BlockSpec((1, 8, span), lambda g, b: (g, 0, 0))
    return pl.pallas_call(
        functools.partial(attn_bwd_kernel, heads=heads, head_dim=head_dim),
        grid=(count, batch),
        in_specs=specs + [pl.BlockSpec((1, seq_len, span), lambda g, b: (b, 0, g + first))],
        out_specs=[pl.BlockSpec((1, seq_len, 3 * span), lambda g, b: (b, 0, g)),
                   pl.BlockSpec((1, seq_len, span), lambda g, b: (g, 0, 0)), vec8, vec8],
        out_shape=[jax.ShapeDtypeStruct((batch, seq_len, 3 * count * span), BF16),
                   jax.ShapeDtypeStruct((count, seq_len, span), F32), small, small],
        scratch_shapes=square(F32, F32, BF16, BF16, BF16, BF16) + [pltpu.VMEM((heads, seq_len, head_dim), BF16)] * 3,
        compiler_params=pltpu.CompilerParams(dimension_semantics=("arbitrary", "arbitrary")),
        cost_estimate=pl.CostEstimate(flops=20 * work, bytes_accessed=14 * batch * seq_len * count * span, transcendentals=0),
        name="attn_bwd",
    )(qkv, rel, bias_u, bias_w, d_ctx)


def interleave_kernel(*refs):
    out_ref = refs[-1]
    for n, ref in enumerate(refs[:-1]):
        width = ref.shape[-1]
        out_ref[..., n * width:(n + 1) * width] = ref[...]


def interleave(arrays, width):
    rows, cols = arrays[0].shape
    spec = pl.BlockSpec((rows, width), lambda i: (0, i))
    total = len(arrays) * cols
    return pl.pallas_call(
        interleave_kernel,
        grid=(cols // width,),
        in_specs=[spec] * len(arrays),
        out_specs=pl.BlockSpec((rows, len(arrays) * width), lambda i: (0, i)),
        out_shape=jax.ShapeDtypeStruct((rows, total), arrays[0].dtype),
        cost_estimate=pl.CostEstimate(flops=rows * total, bytes_accessed=4 * rows * total, transcendentals=0),
        name="interleave",
    )(*arrays)


def separate_kernel(in_ref, out_ref):
    width = out_ref.shape[-1]
    for n in range(out_ref.shape[0]):
        out_ref[n] = in_ref[:, n * width:(n + 1) * width]


def separate(array, count, width):
    rows, cols = array.shape
    return pl.pallas_call(
        separate_kernel,
        grid=(cols // (count * width),),
        in_specs=[pl.BlockSpec((rows, count * width), lambda i: (0, i))],
        out_specs=pl.BlockSpec((count, rows, width), lambda i: (0, 0, i)),
        out_shape=jax.ShapeDtypeStruct((count, rows, cols // count), array.dtype),
        cost_estimate=pl.CostEstimate(flops=rows * cols, bytes_accessed=4 * rows * cols, transcendentals=0),
        name="separate",
    )(array)


def solution(mesh):
    axis_name = mesh.axis_names[0]
    group_size = mesh.shape[axis_name]
    chips = group_size // 2
    pairs = [(d, d ^ 1) for d in range(group_size)]
    same_core = [[2 * c + core for c in range(chips)] for core in range(2)]

    def gather(local_shard):
        return lax.all_gather(local_shard, axis_name, axis=0, tiled=True)

    def local_step(x_in, grad_out, norm_attn, w_query, w_key, w_value, w_rel, bias_u, bias_w, w_attn_out, norm_mlp, w_up, w_down):
        batch_local, seq_len, width = x_in.shape
        num_heads, head_dim = w_query.shape[1], w_query.shape[2]
        hidden = num_heads * head_dim
        tokens = batch_local * seq_len
        span = hidden // group_size
        scale = 1.0 / (batch_local * group_size)
        me = lax.axis_index(axis_name)
        core = lax.rem(me, 2)

        def shares(acts, kind):
            part = acts.shape[1] // group_size
            return jnp.concatenate(
                [lax.dynamic_slice(acts, (0, (2 * c + kind) * part), (tokens, part)) for c in range(chips)], axis=1)

        def theirs(acts, cots):
            mine = dot_tn(shares(acts, 1 - core), cots)
            return mine, lax.ppermute(mine, axis_name, pairs)

        def ours(acts, cots, received):
            return (dot_tn(shares(acts, core), cots) + received) * scale

        def spread(summed):
            return lax.psum_scatter(summed, axis_name, scatter_dimension=0, axis_index_groups=same_core, tiled=True)

        def gather_halves(stacked):
            full = lax.all_gather(stacked, axis_name, axis=1, tiled=True)
            return with_layout_constraint(full, Layout(major_to_minor=(0, 1, 2)))

        x_f32 = x_in.reshape(tokens, width).astype(F32)
        dy = grad_out.reshape(tokens, width)
        vecs = lax.all_gather(jnp.stack([norm_attn, bias_u, bias_w, norm_mlp]), axis_name, axis=0)
        gain_attn = vecs[:, 0].reshape(width).astype(F32)
        u_full = vecs[:, 1:2].astype(F32)
        w_full = vecs[:, 2:3].astype(F32)
        gain_mlp = vecs[:, 3].reshape(width).astype(F32)

        qkv_own = interleave([z.reshape(-1, hidden) for z in (w_query, w_key, w_value)], span)
        qkv_full = gather(qkv_own)

        pos_table = sin_table(seq_len, width)
        rel_rows = after(w_rel, qkv_own).reshape(-1, hidden)
        rel_cols = lax.all_to_all(rel_rows, axis_name, split_axis=1, concat_axis=0, tiled=True)
        rel_own = dot_nn(pos_table, rel_cols).astype(BF16)
        lines = seq_len * span // width
        folded = jnp.concatenate([rel_own[at:at + lines] for at in range(0, seq_len, lines)], axis=1)
        out_rel = lax.all_gather(jnp.concatenate([w_attn_out, folded], axis=0), axis_name, axis=0)
        out_full = out_rel[:, :-lines].reshape(hidden, width)

        ff_half = w_up.shape[1] // 2
        part = ff_half // group_size
        up_own = separate(after(w_up, qkv_own), 2, part)
        up_full = gather_halves(up_own)
        down_full = gather_halves(after(w_down, up_own).reshape(2, part, width))

        h_attn = rms_norm(x_f32, gain_attn)
        shape3 = (batch_local, seq_len, -1)
        qkv = dot_nn(h_attn, qkv_full).astype(BF16).reshape(shape3)
        context = attn_fwd(qkv, out_rel, u_full, w_full, head_dim).reshape(tokens, hidden)
        x1_f32 = (x_f32 + dot_nn(context, out_full)).astype(BF16).astype(F32)
        h_mlp = rms_norm(x1_f32, gain_mlp)

        def feed(acts, weight):
            pre = dot_nn(acts, weight).astype(BF16)
            return pre, gelu_tanh(pre.astype(F32)).astype(BF16)

        def unfeed(cots, weight, pre):
            d_act = dot_nt(cots, weight).astype(BF16)
            return jax.vjp(gelu_tanh, pre.astype(F32))[1](d_act.astype(F32))[0].astype(BF16)

        pre0, act0 = feed(h_mlp, up_full[0])
        sent, got = theirs(act0, dy)
        pre1, act1 = feed(after(h_mlp, sent), up_full[1])
        sum_down0 = ours(after(act0, act1), dy, got)
        sent, got = theirs(act1, after(dy, sum_down0))
        d_pre0 = unfeed(after(dy, sent), down_full[0], pre0)
        sum_down1 = ours(after(act1, d_pre0), dy, got)
        sent, got = theirs(h_mlp, after(d_pre0, sum_down1))
        d_pre1 = unfeed(after(dy, sent), down_full[1], pre1)
        sum_up0 = ours(h_mlp, after(d_pre0, d_pre1), got)
        sent, got = theirs(h_mlp, after(d_pre1, sum_up0))
        d_h_part = dot_nt(after(d_pre0, sent), up_full[0])
        sum_up1 = ours(h_mlp, after(d_pre1, d_h_part), got)
        d_h_mlp = (d_h_part + dot_nt(after(d_pre1, sum_up1), up_full[1])).astype(BF16)
        grad_down = jnp.concatenate([spread(sum_down0), spread(sum_down1)], axis=0)
        grad_up0, grad_up1 = spread(sum_up0), spread(sum_up1)

        d_x1_norm, grad_norm_mlp = jax.vjp(rms_norm, x1_f32, gain_mlp)[1](d_h_mlp)
        d_x1 = (dy.astype(F32) + d_x1_norm).astype(BF16)
        d_context = dot_nt(d_x1, out_full).astype(BF16).reshape(shape3)
        pairs_half = group_size // 2
        d_low, d_rel_low, d_u_low, d_w_low = attn_bwd(
            qkv, out_rel, u_full, w_full, d_context, head_dim, 0, pairs_half)
        d_low = d_low.reshape(tokens, -1)
        sent, got = theirs(h_attn, d_low)
        sent_o, got_o = theirs(context, after(d_x1, sent))
        sum_low = ours(h_attn, after(d_low, sent_o), got)
        d_high, d_rel_high, d_u_high, d_w_high = attn_bwd(
            qkv, out_rel, u_full, w_full, after(d_context, sum_low), head_dim, pairs_half, pairs_half)
        d_high = d_high.reshape(tokens, -1)
        d_rel_own = lax.psum_scatter(
            jnp.concatenate([d_rel_low, d_rel_high], axis=0), axis_name, scatter_dimension=0, tiled=True)[0]
        sent, got = theirs(h_attn, d_high)
        sum_o = ours(context, after(d_x1, sent), got_o)
        sum_high = ours(h_attn, after(d_high, sum_o), got)
        grad_low, grad_high = spread(sum_low), spread(sum_high)
        y_out = (x1_f32 + dot_nn(after(act0, sum_high), down_full[0]) + dot_nn(act1, down_full[1])).astype(BF16)
        d_rel_own = after(d_rel_own, y_out)
        d_rel_own = jnp.flip(d_rel_own.reshape(seq_len // BLK, BLK, span), axis=1).reshape(seq_len, span).astype(BF16)
        d_rel_all = lax.all_gather(d_rel_own, axis_name, axis=0)
        grad_attn_out = spread(after(sum_o, d_rel_own))

        cut = qkv_full.shape[1] // 2
        d_h_attn = (dot_nt(after(d_low, d_rel_own), qkv_full[:, :cut]) + dot_nt(d_high, qkv_full[:, cut:])).astype(BF16)
        d_x_norm, grad_norm_attn = jax.vjp(rms_norm, x_f32, gain_attn)[1](d_h_attn)
        grad_x = (d_x1.astype(F32) + d_x_norm).astype(BF16)

        table_own = lax.dynamic_slice(pos_table, (0, me * (width // group_size)), (seq_len, width // group_size))
        grad_rel = dot_tn(table_own, jnp.swapaxes(d_rel_all, 0, 1).reshape(seq_len, hidden)) * scale
        grad_up = interleave([grad_up0, grad_up1], part)
        grad_parts = [z.reshape(-1, pairs_half, 3, span) for z in (grad_low, grad_high)]
        grad_query, grad_key, grad_value = (
            jnp.concatenate([z[:, :, n] for z in grad_parts], axis=1) for n in range(3))
        d_u = jnp.concatenate([d_u_low, d_u_high], axis=0)
        d_w = jnp.concatenate([d_w_low, d_w_high], axis=0)

        small = jnp.stack([grad_norm_attn.reshape(group_size, span), jnp.sum(d_u, axis=1), jnp.sum(d_w, axis=1),
                           grad_norm_mlp.reshape(group_size, span)], axis=1)
        small = lax.psum_scatter(small * scale, axis_name, scatter_dimension=0, tiled=True)[0]

        heads3 = (-1, num_heads, head_dim)
        return (y_out.reshape(x_in.shape), grad_x.reshape(x_in.shape), small[0], grad_query.reshape(heads3),
                grad_key.reshape(heads3), grad_value.reshape(heads3), grad_rel.reshape(heads3), small[1], small[2],
                grad_attn_out, small[3], grad_up, grad_down)

    sharded = P(axis_name)
    return jax.shard_map(local_step, mesh=mesh, in_specs=(sharded,) * 13, out_specs=(sharded,) * 13, check_vma=False)
```

```python
import functools

import jax
import jax.numpy as jnp
from jax import lax
from jax.experimental import pallas as pl
from jax.experimental.layout import Layout, with_layout_constraint
from jax.experimental.pallas import tpu as pltpu
from jax.sharding import PartitionSpec as P


EPS = 1e-6
MASK_VALUE = -1e30
BLK = 128
SUB = 64
SEQ = 512
F32 = jnp.float32
BF16 = jnp.bfloat16


def sin_table(seq_len, model_width):
    distance = (seq_len - 1 - jnp.arange(seq_len)).astype(F32)
    inv_freq = 10000.0 ** (-jnp.arange(0, model_width, 2).astype(F32) / model_width)
    angles = distance[:, None] * inv_freq[None, :]
    return jnp.concatenate([jnp.sin(angles), jnp.cos(angles)], axis=-1).astype(BF16)


def rms_norm(x_f32, gain_vec):
    mean_sq = jnp.mean(x_f32 * x_f32, axis=-1, keepdims=True)
    return (x_f32 * lax.rsqrt(mean_sq + EPS) * gain_vec).astype(BF16)


def gelu_tanh(pre_f32):
    return jax.nn.gelu(pre_f32, approximate=True)


def dot_nn(a, b):
    return lax.dot_general(a, b, (((1,), (0,)), ((), ())), preferred_element_type=F32)


def dot_nt(a, b):
    return lax.dot_general(a, b, (((1,), (1,)), ((), ())), preferred_element_type=F32)


def dot_tn(a, b):
    return lax.dot_general(a, b, (((0,), (0,)), ((), ())), preferred_element_type=F32)


def after(value, *earlier):
    return lax.optimization_barrier((value, *earlier))[0]


def tril_mask(first):
    shape = (SUB, BLK)
    return lax.broadcasted_iota(jnp.int32, shape, 0) + first >= lax.broadcasted_iota(jnp.int32, shape, 1)


def shear(x, first):
    return pltpu.roll(x, 1 + first, axis=1, stride=1, stride_axis=0)


def halves_of(seq_len):
    half = seq_len // 2
    return [(slice(h * half, (h + 1) * half), (h + 1) * half) for h in range(2)]


def fill_scores(q_u, q_w, keys, rel, s_ref, t_ref):
    seq_len = q_u.shape[0]
    for rows, top in halves_of(seq_len):
        s_ref[rows, :top] = dot_nt(q_u[rows], keys[:top])
        t_ref[rows, :top] = dot_nt(q_w[rows], rel[seq_len - top:])


def row_pieces(seq_len):
    return [(slice(at, at + SUB), at // BLK, at % BLK) for at in range(0, seq_len, SUB)]


def piece_probs(s_ref, t_ref, piece, head_dim):
    rows, block, first = piece
    tril = tril_mask(first)
    skip = 1 - block % 2
    scale = head_dim ** -0.5
    turned = [shear(t_ref[rows, (skip + c) * BLK:(skip + c + 1) * BLK], first) for c in range(block + 1)]
    parts = []
    for c in range(block + 1):
        part = s_ref[rows, c * BLK:(c + 1) * BLK]
        if c < block:
            part = (part + jnp.where(tril, turned[c], turned[c + 1])) * scale
        else:
            part = jnp.where(tril, (part + turned[c]) * scale, MASK_VALUE)
        parts.append(part)
    logits = jnp.concatenate(parts, axis=1) if block else parts[0]
    grown = jnp.exp(logits - jnp.max(logits, axis=1, keepdims=True))
    return grown * (1.0 / jnp.sum(grown, axis=1, keepdims=True))


def put_piece(ref, piece, value, front):
    rows, block, _ = piece
    width = (block + 1) * BLK
    skip = BLK if front and block % 2 == 0 else 0
    ref[rows, skip:skip + width] = value
    if block % 2 == 0:
        rest = 0 if front else width
        ref[rows, rest:rest + BLK] = jnp.zeros((SUB, BLK), ref.dtype)


def unpack_rel(r_ref):
    width = r_ref.shape[1] * r_ref.shape[2] // SEQ
    return jnp.concatenate([r_ref[0, :, at:at + width] for at in range(0, r_ref.shape[2], width)], axis=0)


def attn_fwd_kernel(qkv_ref, r_ref, u_ref, w_ref, c_ref, s_all, t_all, p_all, *, heads, head_dim):
    seq_len = qkv_ref.shape[1]
    q_ref, k_ref, v_ref = (qkv_ref.at[:, :, part * heads * head_dim:(part + 1) * heads * head_dim] for part in range(3))
    rel_pair = unpack_rel(r_ref)
    all_cols = [slice(n * head_dim, (n + 1) * head_dim) for n in range(heads)]
    for n, cols in enumerate(all_cols):
        q_f32 = q_ref[0, :, cols].astype(F32)
        q_u = (q_f32 + u_ref[0, :, cols]).astype(BF16)
        q_w = (q_f32 + w_ref[0, :, cols]).astype(BF16)
        fill_scores(q_u, q_w, k_ref[0, :, cols], rel_pair[:, cols], s_all.at[n], t_all.at[n])
    for piece in row_pieces(seq_len):
        for n in range(heads):
            put_piece(p_all.at[n], piece, piece_probs(s_all.at[n], t_all.at[n], piece, head_dim).astype(BF16), False)
    for n, cols in enumerate(all_cols):
        for rows, top in halves_of(seq_len):
            c_ref[0, rows, cols] = dot_nn(p_all[n, rows, :top], v_ref[0, :top, cols]).astype(BF16)


def attn_bwd_kernel(qkv_ref, r_ref, u_ref, w_ref, dc_ref, dqkv_ref, dr_ref, du_ref, dw_ref,
                    s_all, t_all, dp_all, p_all, ds_all, dt_all, qu_all, qw_all, rb_all, *, heads, head_dim):
    seq_len = qkv_ref.shape[1]
    parts = [slice(part * heads * head_dim, (part + 1) * heads * head_dim) for part in range(3)]
    q_ref, k_ref, v_ref = (qkv_ref.at[:, :, part] for part in parts)
    dq_ref, dk_ref, dv_ref = (dqkv_ref.at[:, :, part] for part in parts)
    rel_pair = unpack_rel(r_ref)
    blocks = seq_len // BLK
    flip = (lax.broadcasted_iota(jnp.int32, (BLK, BLK), 0) + lax.broadcasted_iota(jnp.int32, (BLK, BLK), 1)
            == BLK - 1).astype(F32).astype(BF16)
    scale = head_dim ** -0.5
    all_cols = [slice(n * head_dim, (n + 1) * head_dim) for n in range(heads)]

    @pl.when(pl.program_id(1) == 0)
    def _():
        dr_ref[...] = jnp.zeros_like(dr_ref)
        du_ref[...] = jnp.zeros_like(du_ref)
        dw_ref[...] = jnp.zeros_like(dw_ref)

    for n, cols in enumerate(all_cols):
        q_f32 = q_ref[0, :, cols].astype(F32)
        qu_all[n] = (q_f32 + u_ref[0, :, cols]).astype(BF16)
        qw_all[n] = (q_f32 + w_ref[0, :, cols]).astype(BF16)
        rel = rel_pair[:, cols]
        fill_scores(qu_all[n], qw_all[n], k_ref[0, :, cols], rel, s_all.at[n], t_all.at[n])
        for rows, top in halves_of(seq_len):
            dp_all[n, rows, :top] = dot_nt(dc_ref[0, rows, cols], v_ref[0, :top, cols]).astype(BF16)
        for c in range(blocks):
            rb_all[n, c * BLK:(c + 1) * BLK] = dot_nn(flip, rel[c * BLK:(c + 1) * BLK]).astype(BF16)
    for piece in row_pieces(seq_len):
        for n in range(heads):
            probs = piece_probs(s_all.at[n], t_all.at[n], piece, head_dim)
            d_probs = dp_all[n, piece[0], :(piece[1] + 1) * BLK].astype(F32)
            inner = jnp.sum(probs * d_probs, axis=1, keepdims=True)
            put_piece(p_all.at[n], piece, probs.astype(BF16), False)
            put_piece(ds_all.at[n], piece, (probs * (d_probs - inner) * scale).astype(BF16), False)
    for n in range(heads):
        for rows, top in halves_of(seq_len):
            for c in range(top // BLK):
                t_all[n, rows, c * BLK:(c + 1) * BLK] = dot_nn(ds_all[n, rows, c * BLK:(c + 1) * BLK], flip)
    for piece in row_pieces(seq_len):
        rows, block, first = piece
        tril = tril_mask(first)
        for n in range(heads):
            turned = [shear(t_all[n, rows, c * BLK:(c + 1) * BLK], first) for c in range(block + 1)]
            parts = [jnp.where(tril, turned[c], turned[c - 1] if c else 0.0).astype(BF16) for c in range(block + 1)]
            put_piece(dt_all.at[n], piece, jnp.concatenate(parts, axis=1) if block else parts[0], True)
    (low, near), (high, far) = halves_of(seq_len)
    for n, cols in enumerate(all_cols):
        for rows, top in halves_of(seq_len):
            d_qu = dot_nn(ds_all[n, rows, :top], k_ref[0, :top, cols]).astype(BF16).astype(F32)
            d_qw = dot_nn(dt_all[n, rows, :top], rb_all[n, seq_len - top:]).astype(BF16).astype(F32)
            dq_ref[0, rows, cols] = (d_qu + d_qw).astype(BF16)
            du_ref[0, :, cols] += jnp.sum(d_qu.reshape(-1, 8, head_dim), axis=0)
            dw_ref[0, :, cols] += jnp.sum(d_qw.reshape(-1, 8, head_dim), axis=0)
        for out_ref, left, right in ((dk_ref, ds_all.at[n], qu_all[n]), (dv_ref, p_all.at[n], dc_ref[0, :, cols])):
            whole = dot_tn(left[high, :], right[high])
            out_ref[0, :near, cols] = (whole[:near] + dot_tn(left[low, :near], right[low])).astype(BF16)
            out_ref[0, near:, cols] = whole[near:].astype(BF16)
        dr_ref[0, :, cols] += dot_tn(dt_all[n, high, :], qw_all[n, high])
        dr_ref[0, near:, cols] += dot_tn(dt_all[n, low, :near], qw_all[n, low])


def attn_args(qkv, rel, bias_u, head_dim, first):
    _, seq_len, width = qkv.shape
    groups, _, span = bias_u.shape
    lines = seq_len * span // rel.shape[2]
    at = rel.shape[1] // lines - 1
    specs = [
        pl.BlockSpec((1, seq_len, width // groups), lambda g, b: (b, 0, g + first)),
        pl.BlockSpec((1, lines, rel.shape[2]), lambda g, b: (g + first, at, 0)),
        pl.BlockSpec((1, 1, span), lambda g, b: (g + first, 0, 0)),
        pl.BlockSpec((1, 1, span), lambda g, b: (g + first, 0, 0)),
    ]
    heads = span // head_dim

    def square(*dtypes):
        return [pltpu.VMEM((heads, seq_len, seq_len), dtype) for dtype in dtypes]

    return specs, square, heads, span


def attn_fwd(qkv, rel, bias_u, bias_w, head_dim):
    batch, seq_len, width = qkv.shape
    groups = bias_u.shape[0]
    specs, square, heads, span = attn_args(qkv, rel, bias_u, head_dim, 0)
    work = batch * groups * heads * seq_len * seq_len * head_dim
    return pl.pallas_call(
        functools.partial(attn_fwd_kernel, heads=heads, head_dim=head_dim),
        grid=(groups, batch),
        in_specs=specs,
        out_specs=pl.BlockSpec((1, seq_len, span), lambda g, b: (b, 0, g)),
        out_shape=jax.ShapeDtypeStruct((batch, seq_len, groups * span), BF16),
        scratch_shapes=square(F32, F32, BF16),
        compiler_params=pltpu.CompilerParams(
            dimension_semantics=("arbitrary", "arbitrary")),
        cost_estimate=pl.CostEstimate(flops=8 * work, bytes_accessed=8 * batch * seq_len * width // 3, transcendentals=0),
        name="attn_fwd",
    )(qkv, rel, bias_u, bias_w)


def attn_bwd(qkv, rel, bias_u, bias_w, d_ctx, head_dim, first, count):
    batch, seq_len, _ = qkv.shape
    specs, square, heads, span = attn_args(qkv, rel, bias_u, head_dim, first)
    work = batch * count * heads * seq_len * seq_len * head_dim
    small = jax.ShapeDtypeStruct((count, 8, span), F32)
    vec8 = pl.BlockSpec((1, 8, span), lambda g, b: (g, 0, 0))
    return pl.pallas_call(
        functools.partial(attn_bwd_kernel, heads=heads, head_dim=head_dim),
        grid=(count, batch),
        in_specs=specs + [pl.BlockSpec((1, seq_len, span), lambda g, b: (b, 0, g + first))],
        out_specs=[pl.BlockSpec((1, seq_len, 3 * span), lambda g, b: (b, 0, g)),
                   pl.BlockSpec((1, seq_len, span), lambda g, b: (g, 0, 0)), vec8, vec8],
        out_shape=[jax.ShapeDtypeStruct((batch, seq_len, 3 * count * span), BF16),
                   jax.ShapeDtypeStruct((count, seq_len, span), F32), small, small],
        scratch_shapes=square(F32, F32, BF16, BF16, BF16, BF16) + [pltpu.VMEM((heads, seq_len, head_dim), BF16)] * 3,
        compiler_params=pltpu.CompilerParams(dimension_semantics=("arbitrary", "arbitrary")),
        cost_estimate=pl.CostEstimate(flops=20 * work, bytes_accessed=14 * batch * seq_len * count * span, transcendentals=0),
        name="attn_bwd",
    )(qkv, rel, bias_u, bias_w, d_ctx)


def interleave_kernel(*refs):
    out_ref = refs[-1]
    for n, ref in enumerate(refs[:-1]):
        width = ref.shape[-1]
        out_ref[..., n * width:(n + 1) * width] = ref[...]


def interleave(arrays, width, place=lambda i: i):
    rows, cols = arrays[0].shape
    total = len(arrays) * cols
    return pl.pallas_call(
        interleave_kernel,
        grid=(cols // width,),
        in_specs=[pl.BlockSpec((rows, width), lambda i: (0, place(i)))] * len(arrays),
        out_specs=pl.BlockSpec((rows, len(arrays) * width), lambda i: (0, i)),
        out_shape=jax.ShapeDtypeStruct((rows, total), arrays[0].dtype),
        cost_estimate=pl.CostEstimate(flops=rows * total, bytes_accessed=4 * rows * total, transcendentals=0),
        name="interleave",
    )(*arrays)


def separate_kernel(in_ref, out_ref):
    width = out_ref.shape[-1]
    for n in range(out_ref.shape[0]):
        out_ref[n] = in_ref[:, n * width:(n + 1) * width]


def separate(array, count, width, place=lambda i: i):
    rows, cols = array.shape
    return pl.pallas_call(
        separate_kernel,
        grid=(cols // (count * width),),
        in_specs=[pl.BlockSpec((rows, count * width), lambda i: (0, i))],
        out_specs=pl.BlockSpec((count, rows, width), lambda i: (0, 0, place(i))),
        out_shape=jax.ShapeDtypeStruct((count, rows, cols // count), array.dtype),
        cost_estimate=pl.CostEstimate(flops=rows * cols, bytes_accessed=4 * rows * cols, transcendentals=0),
        name="separate",
    )(array)


def heads_kernel(low_ref, high_ref, *out_refs, span, head_dim):
    rows = low_ref.shape[0]
    per = span // head_dim
    count = low_ref.shape[1] // (len(out_refs) * span)
    heads = 2 * count * per
    for half, ref in enumerate((low_ref, high_ref)):
        for pair in range(count):
            for part, out_ref in enumerate(out_refs):
                for n in range(per):
                    at = (pair * len(out_refs) + part) * span + n * head_dim
                    head = (half * count + pair) * per + n
                    out_ref[pl.ds(head, rows, stride=heads), :] = ref[:, at:at + head_dim]


def to_heads(low, high, span, head_dim):
    rows, cols = low.shape
    heads = 2 * cols // (3 * head_dim)
    step = rows // 4
    return pl.pallas_call(
        functools.partial(heads_kernel, span=span, head_dim=head_dim),
        grid=(4,),
        in_specs=[pl.BlockSpec((step, cols), lambda i: (i, 0))] * 2,
        out_specs=[pl.BlockSpec((step * heads, head_dim), lambda i: (i, 0))] * 3,
        out_shape=[jax.ShapeDtypeStruct((rows * heads, head_dim), F32)] * 3,
        cost_estimate=pl.CostEstimate(flops=2 * rows * cols, bytes_accessed=16 * rows * cols, transcendentals=0),
        name="to_heads",
    )(low, high)


def wgrad_kernel(kind_ref, *refs, chips, scale):
    del kind_ref
    a_refs, (a2_ref, b1_ref, b2_ref, out_ref, t1, t2) = refs[:chips], refs[chips:]

    @pl.when(pl.program_id(0) == 0)
    def _():
        part = a_refs[0].shape[1]
        for c, ref in enumerate(a_refs):
            t1[c * part:(c + 1) * part] = ref[...].T
            t2[c * part:(c + 1) * part] = a2_ref[:, c * part:(c + 1) * part].T

    out_ref[...] = (dot_nn(t1[...], b1_ref[...]) + dot_nn(t2[...], b2_ref[...])) * scale


def wgrad(kind, acts, acts2, cots, cots2, chips, scale, width):
    tokens, cols = acts.shape
    part = cols // (2 * chips)
    rows, total = chips * part, cots.shape[1]
    share = [pl.BlockSpec((tokens, part), lambda j, k, c=c: (0, 2 * c + k[0])) for c in range(chips)]
    whole = pl.BlockSpec((tokens, rows), lambda j, k: (0, 0))
    block = pl.BlockSpec((tokens, width), lambda j, k: (0, j))
    return pl.pallas_call(
        functools.partial(wgrad_kernel, chips=chips, scale=scale),
        grid_spec=pltpu.PrefetchScalarGridSpec(
            num_scalar_prefetch=1,
            grid=(total // width,),
            in_specs=share + [whole, block, block],
            out_specs=pl.BlockSpec((rows, width), lambda j, k: (0, j)),
            scratch_shapes=[pltpu.VMEM((rows, tokens), BF16)] * 2,
        ),
        out_shape=jax.ShapeDtypeStruct((rows, total), F32),
        compiler_params=pltpu.CompilerParams(dimension_semantics=("arbitrary",), vmem_limit_bytes=56 * 2**20),
        cost_estimate=pl.CostEstimate(
            flops=4 * tokens * rows * total, bytes_accessed=4 * (tokens * total + rows * total), transcendentals=0),
        name="wgrad",
    )(kind, *([acts] * chips), acts2, cots, cots2)


def solution(mesh):
    axis_name = mesh.axis_names[0]
    group_size = mesh.shape[axis_name]
    chips = group_size // 2
    pairs = [(d, d ^ 1) for d in range(group_size)]
    same_core = [[2 * c + core for c in range(chips)] for core in range(2)]

    def gather(local_shard):
        return lax.all_gather(local_shard, axis_name, axis=0, tiled=True)

    def local_step(x_in, grad_out, norm_attn, w_query, w_key, w_value, w_rel, bias_u, bias_w, w_attn_out, norm_mlp, w_up, w_down):
        batch_local, seq_len, width = x_in.shape
        num_heads, head_dim = w_query.shape[1], w_query.shape[2]
        hidden = num_heads * head_dim
        tokens = batch_local * seq_len
        span = hidden // group_size
        scale = 1.0 / (batch_local * group_size)
        me = lax.axis_index(axis_name)
        core = lax.rem(me, 2)

        def shares(acts, kind):
            part = acts.shape[1] // group_size
            return jnp.concatenate(
                [lax.dynamic_slice(acts, (0, (2 * c + kind) * part), (tokens, part)) for c in range(chips)], axis=1)

        def block_of(acts, kind):
            half = acts.shape[1] // 2
            return lax.dynamic_slice(acts, (0, kind * half), (tokens, half))

        def swap(value):
            return lax.ppermute(value, axis_name, pairs)

        def theirs(acts, cots, pick=shares):
            mine = dot_tn(pick(acts, 1 - core), cots)
            return mine, swap(mine)

        def ours(acts, cots, received, pick=shares):
            return (dot_tn(pick(acts, core), cots) + received) * scale

        def spread(summed):
            return lax.psum_scatter(summed, axis_name, scatter_dimension=0, axis_index_groups=same_core, tiled=True)

        def gather_halves(stacked, groups=None):
            full = lax.all_gather(stacked, axis_name, axis=1, tiled=True, axis_index_groups=groups)
            return with_layout_constraint(full, Layout(major_to_minor=(0, 1, 2)))

        def by_kind(device):
            return lax.rem(device, 2) * chips + lax.div(device, 2)

        x_f32 = x_in.reshape(tokens, width).astype(F32)
        dy = grad_out.reshape(tokens, width)
        vecs = lax.all_gather(jnp.stack([norm_attn, bias_u, bias_w, norm_mlp]), axis_name, axis=0)
        gain_attn = vecs[:, 0].reshape(width).astype(F32)
        u_full = vecs[:, 1:2].astype(F32)
        w_full = vecs[:, 2:3].astype(F32)
        gain_mlp = vecs[:, 3].reshape(width).astype(F32)

        qkv_own = interleave([z.reshape(-1, hidden) for z in (w_query, w_key, w_value)], span)
        qkv_full = gather(qkv_own)

        ff_half = w_up.shape[1] // 2
        part = ff_half // group_size
        up_own = separate(after(w_up, qkv_own), 2, part, by_kind)

        pos_table = sin_table(seq_len, width)
        rel_rows = after(w_rel, up_own).reshape(-1, hidden)
        rel_cols = lax.all_to_all(rel_rows, axis_name, split_axis=1, concat_axis=0, tiled=True)
        rel_own = dot_nn(pos_table, rel_cols).astype(BF16)
        lines = seq_len * span // width
        folded = jnp.concatenate([rel_own[at:at + lines] for at in range(0, seq_len, lines)], axis=1)
        out_rel = lax.all_gather(jnp.concatenate([w_attn_out, folded], axis=0), axis_name, axis=0)
        out_full = out_rel[:, :-lines].reshape(hidden, width)

        up_full = gather_halves(up_own)
        down_full = gather_halves(after(w_down, up_own).reshape(2, part, width), [same_core[0] + same_core[1]])

        h_attn = rms_norm(x_f32, gain_attn)
        shape3 = (batch_local, seq_len, -1)
        qkv = dot_nn(h_attn, qkv_full).astype(BF16).reshape(shape3)
        context = attn_fwd(qkv, out_rel, u_full, w_full, head_dim).reshape(tokens, hidden)
        x1_f32 = (x_f32 + dot_nn(context, out_full)).astype(BF16).astype(F32)
        h_mlp = rms_norm(x1_f32, gain_mlp)

        def feed(acts, weight):
            pre = dot_nn(acts, weight).astype(BF16)
            return pre, gelu_tanh(pre.astype(F32)).astype(BF16)

        def unfeed(cots, weight, pre):
            d_act = dot_nt(cots, weight).astype(BF16)
            return jax.vjp(gelu_tanh, pre.astype(F32))[1](d_act.astype(F32))[0].astype(BF16)

        pre0, act0 = feed(h_mlp, up_full[0])
        sent, got = theirs(act0, dy, block_of)
        hidden_theirs = swap(shares(h_mlp, 1 - core))
        pre1, act1 = feed(after(h_mlp, sent), up_full[1])
        sum_down0 = ours(after(act0, act1), dy, got, block_of)
        sent, got = theirs(act1, after(dy, sum_down0), block_of)
        d_pre0 = unfeed(after(dy, sent), down_full[0], pre0)
        d_pre0_theirs = swap(d_pre0)
        sum_down1 = ours(after(act1, d_pre0), dy, got, block_of)
        d_pre1 = unfeed(after(dy, sum_down1), down_full[1], pre1)
        d_pre1_theirs = swap(d_pre1)
        kind = core[None]
        sum_up0 = wgrad(kind, h_mlp, hidden_theirs, after(d_pre0, d_pre1), d_pre0_theirs, chips, scale, 512)
        d_h_part = dot_nt(after(d_pre0, sum_up0), up_full[0])
        sum_up1 = wgrad(kind, h_mlp, hidden_theirs, after(d_pre1, d_h_part), d_pre1_theirs, chips, scale, 512)
        d_h_mlp = (d_h_part + dot_nt(after(d_pre1, sum_up1), up_full[1])).astype(BF16)
        grad_down = jnp.concatenate([spread(sum_down0), spread(sum_down1)], axis=0)
        grad_up0, grad_up1 = spread(sum_up0), spread(sum_up1)

        d_x1_norm, grad_norm_mlp = jax.vjp(rms_norm, x1_f32, gain_mlp)[1](d_h_mlp)
        d_x1 = (dy.astype(F32) + d_x1_norm).astype(BF16)
        d_context = dot_nt(d_x1, out_full).astype(BF16).reshape(shape3)
        pairs_half = group_size // 2
        d_low, d_rel_low, d_u_low, d_w_low = attn_bwd(
            qkv, out_rel, u_full, w_full, d_context, head_dim, 0, pairs_half)
        d_low = d_low.reshape(tokens, -1)
        sent, got = theirs(h_attn, d_low)
        sent_o, got_o = theirs(context, after(d_x1, sent))
        sum_low = ours(h_attn, after(d_low, sent_o), got)
        d_high, d_rel_high, d_u_high, d_w_high = attn_bwd(
            qkv, out_rel, u_full, w_full, after(d_context, sum_low), head_dim, pairs_half, pairs_half)
        d_high = d_high.reshape(tokens, -1)
        d_rel = jnp.concatenate([d_rel_low, d_rel_high], axis=0).reshape(chips, 2, seq_len, span)
        got_rel = swap(lax.dynamic_index_in_dim(d_rel, 1 - core, 1, keepdims=False))
        sent, got = theirs(h_attn, d_high)
        sum_o = ours(context, after(d_x1, sent), got_o)
        d_rel = lax.dynamic_index_in_dim(d_rel, core, 1, keepdims=False) + got_rel
        d_rel = jnp.concatenate([d_rel[:, at:at + lines] for at in range(0, seq_len, lines)], axis=2)
        sum_o_rel = jnp.concatenate([sum_o.reshape(chips, -1, width), d_rel], axis=1).reshape(-1, width)
        grad_o_rel = spread(sum_o_rel)
        sum_high = ours(h_attn, after(d_high, sum_o_rel), got)
        grad_low, grad_high = spread(sum_low), spread(sum_high)
        y_out = (x1_f32 + dot_nn(after(act0, sum_high), down_full[0]) + dot_nn(act1, down_full[1])).astype(BF16)

        cut = qkv_full.shape[1] // 2
        d_h_attn = (dot_nt(after(d_low, y_out), qkv_full[:, :cut]) + dot_nt(d_high, qkv_full[:, cut:])).astype(BF16)
        d_x_norm, grad_norm_attn = jax.vjp(rms_norm, x_f32, gain_attn)[1](d_h_attn)
        grad_x = (d_x1.astype(F32) + d_x_norm).astype(BF16)

        grad_o_rel = after(grad_o_rel, d_h_attn)
        grad_attn_out = grad_o_rel[:-lines]
        d_rel_own = jnp.concatenate(
            [grad_o_rel[-lines:, at:at + span] for at in range(0, width, span)], axis=0).reshape(seq_len // BLK, BLK, span)
        d_rel_own = jnp.flip(d_rel_own, axis=1).reshape(1, seq_len, span).astype(BF16)
        d_rel_all = lax.all_to_all(
            jnp.broadcast_to(d_rel_own, (group_size, seq_len, span)), axis_name, split_axis=0, concat_axis=0, tiled=True)
        table_own = lax.dynamic_slice(pos_table, (0, me * (width // group_size)), (seq_len, width // group_size))
        grad_rel = dot_tn(table_own, jnp.swapaxes(d_rel_all, 0, 1).reshape(seq_len, hidden)) * scale
        grad_up = interleave([grad_up0, grad_up1], part, by_kind)
        grad_query, grad_key, grad_value = to_heads(grad_low, grad_high, span, head_dim)
        d_u = jnp.concatenate([d_u_low, d_u_high], axis=0)
        d_w = jnp.concatenate([d_w_low, d_w_high], axis=0)

        small = jnp.stack([grad_norm_attn.reshape(group_size, span), jnp.sum(d_u, axis=1), jnp.sum(d_w, axis=1),
                           grad_norm_mlp.reshape(group_size, span)], axis=1)
        small = lax.psum_scatter(small * scale, axis_name, scatter_dimension=0, tiled=True)[0]

        heads3 = (-1, num_heads, head_dim)
        return (y_out.reshape(x_in.shape), grad_x.reshape(x_in.shape), small[0], grad_query.reshape(heads3),
                grad_key.reshape(heads3), grad_value.reshape(heads3), grad_rel.reshape(heads3), small[1], small[2],
                grad_attn_out, small[3], grad_up, grad_down)

    sharded = P(axis_name)
    return jax.shard_map(local_step, mesh=mesh, in_specs=(sharded,) * 13, out_specs=(sharded,) * 13, check_vma=False)
```

```python
import functools

import jax
import jax.numpy as jnp
from jax import lax
from jax.experimental import pallas as pl
from jax.experimental.layout import Layout, with_layout_constraint
from jax.experimental.pallas import tpu as pltpu
from jax.sharding import PartitionSpec as P


EPS = 1e-6
MASK_VALUE = -1e30
BLK = 128
SUB = 64
SEQ = 512
F32 = jnp.float32
BF16 = jnp.bfloat16


def sin_table(seq_len, model_width):
    distance = (seq_len - 1 - jnp.arange(seq_len)).astype(F32)
    inv_freq = 10000.0 ** (-jnp.arange(0, model_width, 2).astype(F32) / model_width)
    angles = distance[:, None] * inv_freq[None, :]
    return jnp.concatenate([jnp.sin(angles), jnp.cos(angles)], axis=-1).astype(BF16)


def rms_norm(x_f32, gain_vec):
    mean_sq = jnp.mean(x_f32 * x_f32, axis=-1, keepdims=True)
    return (x_f32 * lax.rsqrt(mean_sq + EPS) * gain_vec).astype(BF16)


def gelu_tanh(pre_f32):
    return jax.nn.gelu(pre_f32, approximate=True)


def dot_nn(a, b):
    return lax.dot_general(a, b, (((1,), (0,)), ((), ())), preferred_element_type=F32)


def dot_nt(a, b):
    return lax.dot_general(a, b, (((1,), (1,)), ((), ())), preferred_element_type=F32)


def dot_tn(a, b):
    return lax.dot_general(a, b, (((0,), (0,)), ((), ())), preferred_element_type=F32)


def after(value, *earlier):
    return lax.optimization_barrier((value, *earlier))[0]


def tril_mask(first):
    shape = (SUB, BLK)
    return lax.broadcasted_iota(jnp.int32, shape, 0) + first >= lax.broadcasted_iota(jnp.int32, shape, 1)


def shear(x, first):
    return pltpu.roll(x, 1 + first, axis=1, stride=1, stride_axis=0)


def halves_of(seq_len):
    half = seq_len // 2
    return [(slice(h * half, (h + 1) * half), (h + 1) * half) for h in range(2)]


def fill_scores(q_u, q_w, keys, rel, s_ref, t_ref):
    seq_len = q_u.shape[0]
    for rows, top in halves_of(seq_len):
        s_ref[rows, :top] = dot_nt(q_u[rows], keys[:top])
        t_ref[rows, :top] = dot_nt(q_w[rows], rel[seq_len - top:])


def row_pieces(seq_len):
    return [(slice(at, at + SUB), at // BLK, at % BLK) for at in range(0, seq_len, SUB)]


def piece_probs(s_ref, t_ref, piece, head_dim):
    rows, block, first = piece
    tril = tril_mask(first)
    skip = 1 - block % 2
    scale = head_dim ** -0.5
    turned = [shear(t_ref[rows, (skip + c) * BLK:(skip + c + 1) * BLK], first) for c in range(block + 1)]
    parts = []
    for c in range(block + 1):
        part = s_ref[rows, c * BLK:(c + 1) * BLK]
        if c < block:
            part = (part + jnp.where(tril, turned[c], turned[c + 1])) * scale
        else:
            part = jnp.where(tril, (part + turned[c]) * scale, MASK_VALUE)
        parts.append(part)
    logits = jnp.concatenate(parts, axis=1) if block else parts[0]
    grown = jnp.exp(logits - jnp.max(logits, axis=1, keepdims=True))
    return grown * (1.0 / jnp.sum(grown, axis=1, keepdims=True))


def put_piece(ref, piece, value, front):
    rows, block, _ = piece
    width = (block + 1) * BLK
    skip = BLK if front and block % 2 == 0 else 0
    ref[rows, skip:skip + width] = value
    if block % 2 == 0:
        rest = 0 if front else width
        ref[rows, rest:rest + BLK] = jnp.zeros((SUB, BLK), ref.dtype)


def unpack_rel(r_ref):
    width = r_ref.shape[1] * r_ref.shape[2] // SEQ
    return jnp.concatenate([r_ref[0, :, at:at + width] for at in range(0, r_ref.shape[2], width)], axis=0)


def attn_fwd_kernel(qkv_ref, r_ref, u_ref, w_ref, c_ref, s_all, t_all, p_all, *, heads, head_dim):
    seq_len = qkv_ref.shape[1]
    q_ref, k_ref, v_ref = (qkv_ref.at[:, :, part * heads * head_dim:(part + 1) * heads * head_dim] for part in range(3))
    rel_pair = unpack_rel(r_ref)
    all_cols = [slice(n * head_dim, (n + 1) * head_dim) for n in range(heads)]
    for n, cols in enumerate(all_cols):
        q_f32 = q_ref[0, :, cols].astype(F32)
        q_u = (q_f32 + u_ref[0, :, cols]).astype(BF16)
        q_w = (q_f32 + w_ref[0, :, cols]).astype(BF16)
        fill_scores(q_u, q_w, k_ref[0, :, cols], rel_pair[:, cols], s_all.at[n], t_all.at[n])
    for piece in row_pieces(seq_len):
        for n in range(heads):
            put_piece(p_all.at[n], piece, piece_probs(s_all.at[n], t_all.at[n], piece, head_dim).astype(BF16), False)
    for n, cols in enumerate(all_cols):
        for rows, top in halves_of(seq_len):
            c_ref[0, rows, cols] = dot_nn(p_all[n, rows, :top], v_ref[0, :top, cols]).astype(BF16)


def attn_bwd_kernel(qkv_ref, r_ref, u_ref, w_ref, dc_ref, dqkv_ref, dr_ref, du_ref, dw_ref,
                    s_all, t_all, dp_all, p_all, ds_all, dt_all, qu_all, qw_all, rb_all, *, heads, head_dim):
    seq_len = qkv_ref.shape[1]
    parts = [slice(part * heads * head_dim, (part + 1) * heads * head_dim) for part in range(3)]
    q_ref, k_ref, v_ref = (qkv_ref.at[:, :, part] for part in parts)
    dq_ref, dk_ref, dv_ref = (dqkv_ref.at[:, :, part] for part in parts)
    rel_pair = unpack_rel(r_ref)
    blocks = seq_len // BLK
    flip = (lax.broadcasted_iota(jnp.int32, (BLK, BLK), 0) + lax.broadcasted_iota(jnp.int32, (BLK, BLK), 1)
            == BLK - 1).astype(F32).astype(BF16)
    scale = head_dim ** -0.5
    all_cols = [slice(n * head_dim, (n + 1) * head_dim) for n in range(heads)]

    @pl.when(pl.program_id(1) == 0)
    def _():
        dr_ref[...] = jnp.zeros_like(dr_ref)
        du_ref[...] = jnp.zeros_like(du_ref)
        dw_ref[...] = jnp.zeros_like(dw_ref)

    for n, cols in enumerate(all_cols):
        q_f32 = q_ref[0, :, cols].astype(F32)
        qu_all[n] = (q_f32 + u_ref[0, :, cols]).astype(BF16)
        qw_all[n] = (q_f32 + w_ref[0, :, cols]).astype(BF16)
        rel = rel_pair[:, cols]
        fill_scores(qu_all[n], qw_all[n], k_ref[0, :, cols], rel, s_all.at[n], t_all.at[n])
        for rows, top in halves_of(seq_len):
            dp_all[n, rows, :top] = dot_nt(dc_ref[0, rows, cols], v_ref[0, :top, cols]).astype(BF16)
        for c in range(blocks):
            rb_all[n, c * BLK:(c + 1) * BLK] = dot_nn(flip, rel[c * BLK:(c + 1) * BLK]).astype(BF16)
    for piece in row_pieces(seq_len):
        for n in range(heads):
            probs = piece_probs(s_all.at[n], t_all.at[n], piece, head_dim)
            d_probs = dp_all[n, piece[0], :(piece[1] + 1) * BLK].astype(F32)
            inner = jnp.sum(probs * d_probs, axis=1, keepdims=True)
            put_piece(p_all.at[n], piece, probs.astype(BF16), False)
            put_piece(ds_all.at[n], piece, (probs * (d_probs - inner) * scale).astype(BF16), False)
    for n in range(heads):
        for rows, top in halves_of(seq_len):
            for c in range(top // BLK):
                t_all[n, rows, c * BLK:(c + 1) * BLK] = dot_nn(ds_all[n, rows, c * BLK:(c + 1) * BLK], flip)
    for piece in row_pieces(seq_len):
        rows, block, first = piece
        tril = tril_mask(first)
        for n in range(heads):
            turned = [shear(t_all[n, rows, c * BLK:(c + 1) * BLK], first) for c in range(block + 1)]
            parts = [jnp.where(tril, turned[c], turned[c - 1] if c else 0.0).astype(BF16) for c in range(block + 1)]
            put_piece(dt_all.at[n], piece, jnp.concatenate(parts, axis=1) if block else parts[0], True)
    (low, near), (high, far) = halves_of(seq_len)
    for n, cols in enumerate(all_cols):
        for rows, top in halves_of(seq_len):
            d_qu = dot_nn(ds_all[n, rows, :top], k_ref[0, :top, cols]).astype(BF16).astype(F32)
            d_qw = dot_nn(dt_all[n, rows, :top], rb_all[n, seq_len - top:]).astype(BF16).astype(F32)
            dq_ref[0, rows, cols] = (d_qu + d_qw).astype(BF16)
            du_ref[0, :, cols] += jnp.sum(d_qu.reshape(-1, 8, head_dim), axis=0)
            dw_ref[0, :, cols] += jnp.sum(d_qw.reshape(-1, 8, head_dim), axis=0)
        for out_ref, left, right in ((dk_ref, ds_all.at[n], qu_all[n]), (dv_ref, p_all.at[n], dc_ref[0, :, cols])):
            whole = dot_tn(left[high, :], right[high])
            out_ref[0, :near, cols] = (whole[:near] + dot_tn(left[low, :near], right[low])).astype(BF16)
            out_ref[0, near:, cols] = whole[near:].astype(BF16)
        dr_ref[0, :, cols] += dot_tn(dt_all[n, high, :], qw_all[n, high])
        dr_ref[0, near:, cols] += dot_tn(dt_all[n, low, :near], qw_all[n, low])


def attn_args(qkv, rel, bias_u, head_dim, first):
    _, seq_len, width = qkv.shape
    groups, _, span = bias_u.shape
    lines = seq_len * span // rel.shape[2]
    at = rel.shape[1] // lines - 1
    specs = [
        pl.BlockSpec((1, seq_len, width // groups), lambda g, b: (b, 0, g + first)),
        pl.BlockSpec((1, lines, rel.shape[2]), lambda g, b: (g + first, at, 0)),
        pl.BlockSpec((1, 1, span), lambda g, b: (g + first, 0, 0)),
        pl.BlockSpec((1, 1, span), lambda g, b: (g + first, 0, 0)),
    ]
    heads = span // head_dim

    def square(*dtypes):
        return [pltpu.VMEM((heads, seq_len, seq_len), dtype) for dtype in dtypes]

    return specs, square, heads, span


def attn_fwd(qkv, rel, bias_u, bias_w, head_dim):
    batch, seq_len, width = qkv.shape
    groups = bias_u.shape[0]
    specs, square, heads, span = attn_args(qkv, rel, bias_u, head_dim, 0)
    work = batch * groups * heads * seq_len * seq_len * head_dim
    return pl.pallas_call(
        functools.partial(attn_fwd_kernel, heads=heads, head_dim=head_dim),
        grid=(groups, batch),
        in_specs=specs,
        out_specs=pl.BlockSpec((1, seq_len, span), lambda g, b: (b, 0, g)),
        out_shape=jax.ShapeDtypeStruct((batch, seq_len, groups * span), BF16),
        scratch_shapes=square(F32, F32, BF16),
        compiler_params=pltpu.CompilerParams(
            dimension_semantics=("arbitrary", "arbitrary")),
        cost_estimate=pl.CostEstimate(flops=8 * work, bytes_accessed=8 * batch * seq_len * width // 3, transcendentals=0),
        name="attn_fwd",
    )(qkv, rel, bias_u, bias_w)


def attn_bwd(qkv, rel, bias_u, bias_w, d_ctx, head_dim, first, count):
    batch, seq_len, _ = qkv.shape
    specs, square, heads, span = attn_args(qkv, rel, bias_u, head_dim, first)
    work = batch * count * heads * seq_len * seq_len * head_dim
    small = jax.ShapeDtypeStruct((count, 8, span), F32)
    vec8 = pl.BlockSpec((1, 8, span), lambda g, b: (g, 0, 0))
    return pl.pallas_call(
        functools.partial(attn_bwd_kernel, heads=heads, head_dim=head_dim),
        grid=(count, batch),
        in_specs=specs + [pl.BlockSpec((1, seq_len, span), lambda g, b: (b, 0, g + first))],
        out_specs=[pl.BlockSpec((1, seq_len, 3 * span), lambda g, b: (b, 0, g)),
                   pl.BlockSpec((1, seq_len, span), lambda g, b: (g, 0, 0)), vec8, vec8],
        out_shape=[jax.ShapeDtypeStruct((batch, seq_len, 3 * count * span), BF16),
                   jax.ShapeDtypeStruct((count, seq_len, span), F32), small, small],
        scratch_shapes=square(F32, F32, BF16, BF16, BF16, BF16) + [pltpu.VMEM((heads, seq_len, head_dim), BF16)] * 3,
        compiler_params=pltpu.CompilerParams(dimension_semantics=("arbitrary", "arbitrary")),
        cost_estimate=pl.CostEstimate(flops=20 * work, bytes_accessed=14 * batch * seq_len * count * span, transcendentals=0),
        name="attn_bwd",
    )(qkv, rel, bias_u, bias_w, d_ctx)


def interleave_kernel(*refs):
    out_ref = refs[-1]
    for n, ref in enumerate(refs[:-1]):
        width = ref.shape[-1]
        out_ref[..., n * width:(n + 1) * width] = ref[...]


def interleave(arrays, width, blocks, places=None):
    rows = arrays[0].shape[0]
    places = places or [lambda i: i] * len(arrays)
    total = len(arrays) * width * blocks
    return pl.pallas_call(
        interleave_kernel,
        grid=(blocks,),
        in_specs=[pl.BlockSpec((rows, width), lambda i, f=f: (0, f(i))) for f in places],
        out_specs=pl.BlockSpec((rows, len(arrays) * width), lambda i: (0, i)),
        out_shape=jax.ShapeDtypeStruct((rows, total), arrays[0].dtype),
        cost_estimate=pl.CostEstimate(flops=rows * total, bytes_accessed=4 * rows * total, transcendentals=0),
        name="interleave",
    )(*arrays)


def separate_kernel(in_ref, out_ref):
    width = out_ref.shape[-1]
    for n in range(out_ref.shape[0]):
        out_ref[n] = in_ref[:, n * width:(n + 1) * width]


def separate(array, count, width, place=lambda i: i):
    rows, cols = array.shape
    return pl.pallas_call(
        separate_kernel,
        grid=(cols // (count * width),),
        in_specs=[pl.BlockSpec((rows, count * width), lambda i: (0, i))],
        out_specs=pl.BlockSpec((count, rows, width), lambda i: (0, 0, place(i))),
        out_shape=jax.ShapeDtypeStruct((count, rows, cols // count), array.dtype),
        cost_estimate=pl.CostEstimate(flops=rows * cols, bytes_accessed=4 * rows * cols, transcendentals=0),
        name="separate",
    )(array)


def heads_kernel(in_ref, *out_refs, span, head_dim):
    rows, cols = in_ref.shape
    heads = cols // (len(out_refs) * head_dim)
    per = span // head_dim
    for head in range(heads):
        for part, out_ref in enumerate(out_refs):
            at = (head // per * len(out_refs) + part) * span + head % per * head_dim
            out_ref[pl.ds(head, rows, stride=heads), :] = in_ref[:, at:at + head_dim]


def to_heads(array, span, head_dim):
    rows, cols = array.shape
    heads = cols // (3 * head_dim)
    step = rows // 4
    return pl.pallas_call(
        functools.partial(heads_kernel, span=span, head_dim=head_dim),
        grid=(4,),
        in_specs=[pl.BlockSpec((step, cols), lambda i: (i, 0))],
        out_specs=[pl.BlockSpec((step * heads, head_dim), lambda i: (i, 0))] * 3,
        out_shape=[jax.ShapeDtypeStruct((rows * heads, head_dim), F32)] * 3,
        cost_estimate=pl.CostEstimate(flops=rows * cols, bytes_accessed=8 * rows * cols, transcendentals=0),
        name="to_heads",
    )(array)


def wgrad_kernel(kind_ref, *refs, count, scale, blank):
    del kind_ref
    a_refs, (a2_ref, b1_ref, b2_ref) = refs[:count], refs[count:count + 3]
    out_ref, t1, t2 = refs[count + 3 + blank:]

    @pl.when(pl.program_id(1) == 0)
    def _():
        part = a_refs[0].shape[1]
        for c, ref in enumerate(a_refs):
            t1[c * part:(c + 1) * part] = ref[...].T
            t2[c * part:(c + 1) * part] = a2_ref[:, c * part:(c + 1) * part].T

    total = (dot_nn(t1[...], b1_ref[...]) + dot_nn(t2[...], b2_ref[...])) * scale
    out_ref[...] = total.reshape(out_ref.shape)


def wgrad(kind, acts, acts2, cots, cots2, chips, scale, spread=True, place=(None, None), into=None):
    tokens, cols = acts.shape
    width, tile, depth = 512, 1024, cols // 2
    tiles = depth // tile
    if spread:
        part = tile // chips
        share = [pl.BlockSpec((tokens, part), lambda i, j, k, c=c: (0, 2 * c + k[0])) for c in range(chips)]
    else:
        share = [pl.BlockSpec((tokens, tile), lambda i, j, k: (0, tiles * k[0] + i))]
    block = pl.BlockSpec((tokens, width), lambda i, j, k: (0, j))
    specs = share + [pl.BlockSpec((tokens, tile), lambda i, j, k: (0, i)), block, block]
    args = [acts] * len(share) + [acts2, cots, cots2]
    at, aliases = 0, {}
    if into is not None:
        specs.append(pl.BlockSpec(memory_space=pl.ANY))
        args.append(into[0])
        at, aliases = into[1] // width, {len(args): 0}
    rows, total = place[0], place[1] or cots.shape[1]
    if rows is None:
        out_spec = pl.BlockSpec((tile, width), lambda i, j, k: (i, j + at))
        shape = (depth, total)
    else:
        out_spec = pl.BlockSpec((chips, tile // chips, width), lambda i, j, k: (0, 0, j + at))
        shape = (chips, rows, total)
    return pl.pallas_call(
        functools.partial(wgrad_kernel, count=len(share), scale=scale, blank=int(into is not None)),
        grid_spec=pltpu.PrefetchScalarGridSpec(
            num_scalar_prefetch=1,
            grid=(tiles, cots.shape[1] // width),
            in_specs=specs,
            out_specs=out_spec,
            scratch_shapes=[pltpu.VMEM((tile, tokens), BF16)] * 2,
        ),
        out_shape=jax.ShapeDtypeStruct(shape, F32),
        input_output_aliases=aliases,
        compiler_params=pltpu.CompilerParams(
            dimension_semantics=("arbitrary", "arbitrary"), vmem_limit_bytes=56 * 2**20),
        cost_estimate=pl.CostEstimate(
            flops=4 * tokens * depth * cots.shape[1],
            bytes_accessed=4 * cots.shape[1] * (tokens * tiles + depth), transcendentals=0),
        name="wgrad",
    )(kind, *args)


def solution(mesh):
    axis_name = mesh.axis_names[0]
    group_size = mesh.shape[axis_name]
    chips = group_size // 2
    pairs = [(d, d ^ 1) for d in range(group_size)]
    same_core = [[2 * c + core for c in range(chips)] for core in range(2)]

    def gather(local_shard):
        return lax.all_gather(local_shard, axis_name, axis=0, tiled=True)

    def local_step(x_in, grad_out, norm_attn, w_query, w_key, w_value, w_rel, bias_u, bias_w, w_attn_out, norm_mlp, w_up, w_down):
        batch_local, seq_len, width = x_in.shape
        num_heads, head_dim = w_query.shape[1], w_query.shape[2]
        hidden = num_heads * head_dim
        tokens = batch_local * seq_len
        span = hidden // group_size
        scale = 1.0 / (batch_local * group_size)
        me = lax.axis_index(axis_name)
        core = lax.rem(me, 2)

        def shares(acts, kind):
            part = acts.shape[1] // group_size
            return jnp.concatenate(
                [lax.dynamic_slice(acts, (0, (2 * c + kind) * part), (tokens, part)) for c in range(chips)], axis=1)

        def block_of(acts, kind):
            half = acts.shape[1] // 2
            return lax.dynamic_slice(acts, (0, kind * half), (tokens, half))

        def swap(value):
            return lax.ppermute(value, axis_name, pairs)

        def spread(summed):
            return lax.psum_scatter(summed, axis_name, scatter_dimension=0, axis_index_groups=same_core, tiled=True)

        def gather_halves(stacked, groups=None):
            full = lax.all_gather(stacked, axis_name, axis=1, tiled=True, axis_index_groups=groups)
            return with_layout_constraint(full, Layout(major_to_minor=(0, 1, 2)))

        def by_kind(device):
            return lax.rem(device, 2) * chips + lax.div(device, 2)

        x_f32 = x_in.reshape(tokens, width).astype(F32)
        dy = grad_out.reshape(tokens, width)
        vecs = lax.all_gather(jnp.stack([norm_attn, bias_u, bias_w, norm_mlp]), axis_name, axis=0)
        gain_attn = vecs[:, 0].reshape(width).astype(F32)
        u_full = vecs[:, 1:2].astype(F32)
        w_full = vecs[:, 2:3].astype(F32)
        gain_mlp = vecs[:, 3].reshape(width).astype(F32)

        qkv_own = interleave([z.reshape(-1, hidden) for z in (w_query, w_key, w_value)], span, group_size)
        qkv_full = gather(qkv_own)

        ff_half = w_up.shape[1] // 2
        part = ff_half // group_size
        up_own = separate(after(w_up, qkv_own), 2, part, by_kind)

        pos_table = sin_table(seq_len, width)
        rel_rows = after(w_rel, up_own).reshape(-1, hidden)
        rel_cols = lax.all_to_all(rel_rows, axis_name, split_axis=1, concat_axis=0, tiled=True)
        rel_own = dot_nn(pos_table, rel_cols).astype(BF16)
        lines = seq_len * span // width
        folded = jnp.concatenate([rel_own[at:at + lines] for at in range(0, seq_len, lines)], axis=1)
        out_rel = lax.all_gather(jnp.concatenate([w_attn_out, folded], axis=0), axis_name, axis=0)
        out_full = out_rel[:, :-lines].reshape(hidden, width)

        up_full = gather_halves(up_own)
        down_full = gather_halves(after(w_down, up_own).reshape(2, part, width), [same_core[0] + same_core[1]])

        h_attn = rms_norm(x_f32, gain_attn)
        shape3 = (batch_local, seq_len, -1)
        qkv = dot_nn(h_attn, qkv_full).astype(BF16).reshape(shape3)
        context = attn_fwd(qkv, out_rel, u_full, w_full, head_dim).reshape(tokens, hidden)
        x1_f32 = (x_f32 + dot_nn(context, out_full)).astype(BF16).astype(F32)
        h_mlp = rms_norm(x1_f32, gain_mlp)

        def feed(acts, weight):
            pre = dot_nn(acts, weight).astype(BF16)
            return pre, gelu_tanh(pre.astype(F32)).astype(BF16)

        def unfeed(cots, weight, pre):
            d_act = dot_nt(cots, weight).astype(BF16)
            return jax.vjp(gelu_tanh, pre.astype(F32))[1](d_act.astype(F32))[0].astype(BF16)

        kind = core[None]
        dy_theirs = swap(after(dy, h_attn))
        attn_theirs = swap(shares(after(h_attn, qkv), 1 - core))
        context_theirs = swap(shares(after(context, x1_f32), 1 - core))

        pre0, act0 = feed(h_mlp, up_full[0])
        act0_theirs = swap(block_of(act0, 1 - core))
        pre1, act1 = feed(after(h_mlp, act0), up_full[1])
        sum_down0 = wgrad(kind, after(act0, act1), act0_theirs, dy, dy_theirs, chips, scale, False)
        act1_theirs = swap(block_of(after(act1, sum_down0), 1 - core))
        d_pre0 = unfeed(after(dy, sum_down0), down_full[0], pre0)
        d_pre0_theirs = swap(d_pre0)
        hidden_theirs = swap(shares(h_mlp, 1 - core))
        sum_down1 = wgrad(kind, after(act1, d_pre0), act1_theirs, dy, dy_theirs, chips, scale, False)
        d_pre1 = unfeed(after(dy, sum_down1), down_full[1], pre1)
        d_pre1_theirs = swap(d_pre1)
        both = (None, 2 * ff_half)
        sum_up = wgrad(kind, h_mlp, hidden_theirs, after(d_pre0, d_pre1), d_pre0_theirs, chips, scale,
                       place=both)
        sum_up = wgrad(kind, h_mlp, hidden_theirs, d_pre1, d_pre1_theirs, chips, scale,
                       place=both, into=(sum_up, ff_half))
        d_h_part = dot_nt(after(d_pre0, sum_up), up_full[0])
        d_h_mlp = (d_h_part + dot_nt(after(d_pre1, d_h_part), up_full[1])).astype(BF16)
        grad_down = jnp.concatenate([spread(sum_down0), spread(sum_down1)], axis=0)
        grad_up = spread(sum_up)

        d_x1_norm, grad_norm_mlp = jax.vjp(rms_norm, x1_f32, gain_mlp)[1](d_h_mlp)
        d_x1 = (dy.astype(F32) + d_x1_norm).astype(BF16)
        d_x1_theirs = swap(d_x1)
        d_context = dot_nt(d_x1, out_full).astype(BF16).reshape(shape3)
        d_qkv, d_rel, d_u, d_w = attn_bwd(
            qkv, out_rel, u_full, w_full, d_context, head_dim, 0, group_size)
        d_qkv = d_qkv.reshape(tokens, -1)
        d_qkv_theirs = swap(d_qkv)
        d_rel = d_rel.reshape(chips, 2, seq_len, span)
        got_rel = swap(lax.dynamic_index_in_dim(d_rel, 1 - core, 1, keepdims=False))
        rows = hidden // group_size
        sum_o = wgrad(kind, context, context_theirs, after(d_x1, d_qkv), d_x1_theirs, chips, scale,
                      place=(rows + lines, None))
        d_rel = lax.dynamic_index_in_dim(d_rel, core, 1, keepdims=False) + got_rel
        d_rel = jnp.concatenate([d_rel[:, at:at + lines] for at in range(0, seq_len, lines)], axis=2)
        sum_o = lax.dynamic_update_slice(sum_o, d_rel, (0, rows, 0)).reshape(-1, width)
        grad_o_rel = spread(sum_o)
        sum_qkv = wgrad(kind, h_attn, attn_theirs, after(d_qkv, sum_o), d_qkv_theirs, chips, scale)
        grad_qkv = spread(sum_qkv)
        y_out = (x1_f32 + dot_nn(after(act0, sum_qkv), down_full[0]) + dot_nn(act1, down_full[1])).astype(BF16)

        d_h_attn = dot_nt(after(d_qkv, y_out), qkv_full).astype(BF16)
        d_x_norm, grad_norm_attn = jax.vjp(rms_norm, x_f32, gain_attn)[1](d_h_attn)
        grad_x = (d_x1.astype(F32) + d_x_norm).astype(BF16)

        grad_o_rel = after(grad_o_rel, d_h_attn)
        grad_attn_out = grad_o_rel[:-lines]
        d_rel_own = jnp.concatenate(
            [grad_o_rel[-lines:, at:at + span] for at in range(0, width, span)], axis=0).reshape(seq_len // BLK, BLK, span)
        d_rel_own = jnp.flip(d_rel_own, axis=1).reshape(1, seq_len, span).astype(BF16)
        d_rel_same = lax.all_to_all(
            jnp.broadcast_to(d_rel_own, (chips, seq_len, span)), axis_name, split_axis=0, concat_axis=0, tiled=True,
            axis_index_groups=same_core)
        d_rel_other = swap(d_rel_same)
        d_rel_all = jnp.stack(
            [jnp.where(core == 0, d_rel_same, d_rel_other), jnp.where(core == 0, d_rel_other, d_rel_same)], axis=1)
        table_own = lax.dynamic_slice(pos_table, (0, me * (width // group_size)), (seq_len, width // group_size))
        grad_rel = dot_tn(table_own, d_rel_all.transpose(2, 0, 1, 3).reshape(seq_len, hidden)) * scale
        grad_up = interleave([grad_up, grad_up], part, group_size, [by_kind, lambda d: by_kind(d) + group_size])
        grad_query, grad_key, grad_value = to_heads(grad_qkv, span, head_dim)

        small = jnp.stack([grad_norm_attn.reshape(group_size, span), jnp.sum(d_u, axis=1), jnp.sum(d_w, axis=1),
                           grad_norm_mlp.reshape(group_size, span)], axis=1)
        small = lax.psum_scatter(small * scale, axis_name, scatter_dimension=0, tiled=True)[0]

        heads3 = (-1, num_heads, head_dim)
        return (y_out.reshape(x_in.shape), grad_x.reshape(x_in.shape), small[0], grad_query.reshape(heads3),
                grad_key.reshape(heads3), grad_value.reshape(heads3), grad_rel.reshape(heads3), small[1], small[2],
                grad_attn_out, small[3], grad_up, grad_down)

    sharded = P(axis_name)
    return jax.shard_map(local_step, mesh=mesh, in_specs=(sharded,) * 13, out_specs=(sharded,) * 13, check_vma=False)
```

```python
import functools

import jax
import jax.numpy as jnp
from jax import lax
from jax.experimental import pallas as pl
from jax.experimental.layout import Layout, with_layout_constraint
from jax.experimental.pallas import tpu as pltpu
from jax.sharding import PartitionSpec as P


EPS = 1e-6
MASK_VALUE = -1e30
BLK = 128
SUB = 64
F32 = jnp.float32
BF16 = jnp.bfloat16


def sin_table(seq_len, model_width):
    distance = (seq_len - 1 - jnp.arange(seq_len)).astype(F32)
    inv_freq = 10000.0 ** (-jnp.arange(0, model_width, 2).astype(F32) / model_width)
    angles = distance[:, None] * inv_freq[None, :]
    return jnp.concatenate([jnp.sin(angles), jnp.cos(angles)], axis=-1).astype(BF16)


def rms_norm(x_f32, gain_vec):
    mean_sq = jnp.mean(x_f32 * x_f32, axis=-1, keepdims=True)
    return (x_f32 * lax.rsqrt(mean_sq + EPS) * gain_vec).astype(BF16)


def gelu_tanh(pre_f32):
    return jax.nn.gelu(pre_f32, approximate=True)


def gelu_slope(x):
    c, k = (2.0 / jnp.pi) ** 0.5, 0.044715
    square = x * x
    scaled = c * x
    t = jnp.tanh(scaled * (1.0 + k * square))
    return 0.5 * ((1.0 + t) + (scaled * (1.0 - t * t)) * (1.0 + (3.0 * k) * square))


def dot_nn(a, b):
    return lax.dot_general(a, b, (((1,), (0,)), ((), ())), preferred_element_type=F32)


def dot_nt(a, b):
    return lax.dot_general(a, b, (((1,), (1,)), ((), ())), preferred_element_type=F32)


def dot_tn(a, b):
    return lax.dot_general(a, b, (((0,), (0,)), ((), ())), preferred_element_type=F32)


def after(value, *earlier):
    return lax.optimization_barrier((value, *earlier))[0]


def tril_mask(first):
    shape = (SUB, BLK)
    return lax.broadcasted_iota(jnp.int32, shape, 0) + first >= lax.broadcasted_iota(jnp.int32, shape, 1)


def shear(x, first):
    return pltpu.roll(x, 1 + first, axis=1, stride=1, stride_axis=0)


def halves_of(seq_len):
    half = seq_len // 2
    return [(slice(h * half, (h + 1) * half), (h + 1) * half) for h in range(2)]


def fill_scores(q_u, q_w, keys, rel, s_ref, t_ref):
    seq_len = q_u.shape[0]
    for rows, top in halves_of(seq_len):
        s_ref[rows, :top] = dot_nt(q_u[rows], keys[:top])
        t_ref[rows, :top] = dot_nt(q_w[rows], rel[seq_len - top:])


def row_pieces(seq_len):
    return [(slice(at, at + SUB), at // BLK, at % BLK) for at in range(0, seq_len, SUB)]


def piece_probs(s_ref, t_ref, piece, head_dim):
    rows, block, first = piece
    tril = tril_mask(first)
    skip = 1 - block % 2
    scale = head_dim ** -0.5
    turned = [shear(t_ref[rows, (skip + c) * BLK:(skip + c + 1) * BLK], first) for c in range(block + 1)]
    parts = []
    for c in range(block + 1):
        part = s_ref[rows, c * BLK:(c + 1) * BLK]
        if c < block:
            part = (part + jnp.where(tril, turned[c], turned[c + 1])) * scale
        else:
            part = jnp.where(tril, (part + turned[c]) * scale, MASK_VALUE)
        parts.append(part)
    logits = jnp.concatenate(parts, axis=1) if block else parts[0]
    grown = jnp.exp(logits - jnp.max(logits, axis=1, keepdims=True))
    return grown * (1.0 / jnp.sum(grown, axis=1, keepdims=True))


def put_piece(ref, piece, value, front):
    rows, block, _ = piece
    width = (block + 1) * BLK
    skip = BLK if front and block % 2 == 0 else 0
    ref[rows, skip:skip + width] = value
    if block % 2 == 0:
        rest = 0 if front else width
        ref[rows, rest:rest + BLK] = jnp.zeros((SUB, BLK), ref.dtype)


def attn_fwd_kernel(qkv_ref, r_ref, u_ref, w_ref, c_ref, s_all, t_all, p_all, *, heads, head_dim):
    seq_len = qkv_ref.shape[1]
    q_ref, k_ref, v_ref = (qkv_ref.at[:, :, part * heads * head_dim:(part + 1) * heads * head_dim] for part in range(3))
    rel_pair = r_ref[0]
    all_cols = [slice(n * head_dim, (n + 1) * head_dim) for n in range(heads)]
    for n, cols in enumerate(all_cols):
        q_f32 = q_ref[0, :, cols].astype(F32)
        q_u = (q_f32 + u_ref[0, :, cols]).astype(BF16)
        q_w = (q_f32 + w_ref[0, :, cols]).astype(BF16)
        fill_scores(q_u, q_w, k_ref[0, :, cols], rel_pair[:, cols], s_all.at[n], t_all.at[n])
    for piece in row_pieces(seq_len):
        for n in range(heads):
            put_piece(p_all.at[n], piece, piece_probs(s_all.at[n], t_all.at[n], piece, head_dim).astype(BF16), False)
    for n, cols in enumerate(all_cols):
        for rows, top in halves_of(seq_len):
            c_ref[0, rows, cols] = dot_nn(p_all[n, rows, :top], v_ref[0, :top, cols]).astype(BF16)


def attn_bwd_kernel(qkv_ref, r_ref, u_ref, w_ref, dc_ref, dqkv_ref, dr_ref, du_ref, dw_ref,
                    s_all, t_all, dp_all, p_all, ds_all, dt_all, qu_all, qw_all, rb_all, *, heads, head_dim):
    seq_len = qkv_ref.shape[1]
    parts = [slice(part * heads * head_dim, (part + 1) * heads * head_dim) for part in range(3)]
    q_ref, k_ref, v_ref = (qkv_ref.at[:, :, part] for part in parts)
    dq_ref, dk_ref, dv_ref = (dqkv_ref.at[:, :, part] for part in parts)
    rel_pair = r_ref[0]
    blocks = seq_len // BLK
    flip = (lax.broadcasted_iota(jnp.int32, (BLK, BLK), 0) + lax.broadcasted_iota(jnp.int32, (BLK, BLK), 1)
            == BLK - 1).astype(F32).astype(BF16)
    scale = head_dim ** -0.5
    all_cols = [slice(n * head_dim, (n + 1) * head_dim) for n in range(heads)]

    @pl.when(pl.program_id(1) == 0)
    def _():
        dr_ref[...] = jnp.zeros_like(dr_ref)
        du_ref[...] = jnp.zeros_like(du_ref)
        dw_ref[...] = jnp.zeros_like(dw_ref)

    for n, cols in enumerate(all_cols):
        q_f32 = q_ref[0, :, cols].astype(F32)
        qu_all[n] = (q_f32 + u_ref[0, :, cols]).astype(BF16)
        qw_all[n] = (q_f32 + w_ref[0, :, cols]).astype(BF16)
        rel = rel_pair[:, cols]
        fill_scores(qu_all[n], qw_all[n], k_ref[0, :, cols], rel, s_all.at[n], t_all.at[n])
        for rows, top in halves_of(seq_len):
            dp_all[n, rows, :top] = dot_nt(dc_ref[0, rows, cols], v_ref[0, :top, cols]).astype(BF16)
        for c in range(blocks):
            rb_all[n, c * BLK:(c + 1) * BLK] = dot_nn(flip, rel[c * BLK:(c + 1) * BLK]).astype(BF16)
    for piece in row_pieces(seq_len):
        for n in range(heads):
            probs = piece_probs(s_all.at[n], t_all.at[n], piece, head_dim)
            d_probs = dp_all[n, piece[0], :(piece[1] + 1) * BLK].astype(F32)
            inner = jnp.sum(probs * d_probs, axis=1, keepdims=True)
            put_piece(p_all.at[n], piece, probs.astype(BF16), False)
            put_piece(ds_all.at[n], piece, (probs * (d_probs - inner) * scale).astype(BF16), False)
    for n in range(heads):
        for rows, top in halves_of(seq_len):
            for c in range(top // BLK):
                t_all[n, rows, c * BLK:(c + 1) * BLK] = dot_nn(ds_all[n, rows, c * BLK:(c + 1) * BLK], flip)
    for piece in row_pieces(seq_len):
        rows, block, first = piece
        tril = tril_mask(first)
        for n in range(heads):
            turned = [shear(t_all[n, rows, c * BLK:(c + 1) * BLK], first) for c in range(block + 1)]
            parts = [jnp.where(tril, turned[c], turned[c - 1] if c else 0.0).astype(BF16) for c in range(block + 1)]
            put_piece(dt_all.at[n], piece, jnp.concatenate(parts, axis=1) if block else parts[0], True)
    (low, near), (high, far) = halves_of(seq_len)
    for n, cols in enumerate(all_cols):
        for rows, top in halves_of(seq_len):
            d_qu = dot_nn(ds_all[n, rows, :top], k_ref[0, :top, cols]).astype(BF16).astype(F32)
            d_qw = dot_nn(dt_all[n, rows, :top], rb_all[n, seq_len - top:]).astype(BF16).astype(F32)
            dq_ref[0, rows, cols] = (d_qu + d_qw).astype(BF16)
            du_ref[0, :, cols] += jnp.sum(d_qu.reshape(-1, 8, head_dim), axis=0)
            dw_ref[0, :, cols] += jnp.sum(d_qw.reshape(-1, 8, head_dim), axis=0)
        for out_ref, left, right in ((dk_ref, ds_all.at[n], qu_all[n]), (dv_ref, p_all.at[n], dc_ref[0, :, cols])):
            whole = dot_tn(left[high, :], right[high])
            out_ref[0, :near, cols] = (whole[:near] + dot_tn(left[low, :near], right[low])).astype(BF16)
            out_ref[0, near:, cols] = whole[near:].astype(BF16)
        dr_ref[0, :, cols] += dot_tn(dt_all[n, high, :], qw_all[n, high])
        dr_ref[0, near:, cols] += dot_tn(dt_all[n, low, :near], qw_all[n, low])


def attn_args(qkv, bias_u, head_dim, first):
    _, seq_len, width = qkv.shape
    groups, _, span = bias_u.shape
    specs = [
        pl.BlockSpec((1, seq_len, width // groups), lambda g, b: (b, 0, g + first)),
        pl.BlockSpec((1, seq_len, span), lambda g, b: (g + first, 0, 0)),
        pl.BlockSpec((1, 1, span), lambda g, b: (g + first, 0, 0)),
        pl.BlockSpec((1, 1, span), lambda g, b: (g + first, 0, 0)),
    ]
    heads = span // head_dim

    def square(*dtypes):
        return [pltpu.VMEM((heads, seq_len, seq_len), dtype) for dtype in dtypes]

    return specs, square, heads, span


def attn_fwd(qkv, rel, bias_u, bias_w, head_dim):
    batch, seq_len, width = qkv.shape
    groups = bias_u.shape[0]
    specs, square, heads, span = attn_args(qkv, bias_u, head_dim, 0)
    work = batch * groups * heads * seq_len * seq_len * head_dim
    return pl.pallas_call(
        functools.partial(attn_fwd_kernel, heads=heads, head_dim=head_dim),
        grid=(groups, batch),
        in_specs=specs,
        out_specs=pl.BlockSpec((1, seq_len, span), lambda g, b: (b, 0, g)),
        out_shape=jax.ShapeDtypeStruct((batch, seq_len, groups * span), BF16),
        scratch_shapes=square(F32, F32, BF16),
        compiler_params=pltpu.CompilerParams(
            dimension_semantics=("arbitrary", "arbitrary")),
        cost_estimate=pl.CostEstimate(flops=8 * work, bytes_accessed=8 * batch * seq_len * width // 3, transcendentals=0),
        name="attn_fwd",
    )(qkv, rel, bias_u, bias_w)


def attn_bwd(qkv, rel, bias_u, bias_w, d_ctx, head_dim, first, count):
    batch, seq_len, _ = qkv.shape
    specs, square, heads, span = attn_args(qkv, bias_u, head_dim, first)
    work = batch * count * heads * seq_len * seq_len * head_dim
    small = jax.ShapeDtypeStruct((count, 8, span), F32)
    vec8 = pl.BlockSpec((1, 8, span), lambda g, b: (g, 0, 0))
    return pl.pallas_call(
        functools.partial(attn_bwd_kernel, heads=heads, head_dim=head_dim),
        grid=(count, batch),
        in_specs=specs + [pl.BlockSpec((1, seq_len, span), lambda g, b: (b, 0, g + first))],
        out_specs=[pl.BlockSpec((1, seq_len, 3 * span), lambda g, b: (b, 0, g)),
                   pl.BlockSpec((1, seq_len, span), lambda g, b: (g, 0, 0)), vec8, vec8],
        out_shape=[jax.ShapeDtypeStruct((batch, seq_len, 3 * count * span), BF16),
                   jax.ShapeDtypeStruct((count, seq_len, span), F32), small, small],
        scratch_shapes=square(F32, F32, BF16, BF16, BF16, BF16) + [pltpu.VMEM((heads, seq_len, head_dim), BF16)] * 3,
        compiler_params=pltpu.CompilerParams(dimension_semantics=("arbitrary", "arbitrary")),
        cost_estimate=pl.CostEstimate(flops=20 * work, bytes_accessed=14 * batch * seq_len * count * span, transcendentals=0),
        name="attn_bwd",
    )(qkv, rel, bias_u, bias_w, d_ctx)


def interleave_kernel(*refs):
    out_ref = refs[-1]
    for n, ref in enumerate(refs[:-1]):
        width = ref.shape[-1]
        out_ref[..., n * width:(n + 1) * width] = ref[...]


def interleave(arrays, width, blocks, places=None):
    rows = arrays[0].shape[0]
    places = places or [lambda i: i] * len(arrays)
    total = len(arrays) * width * blocks
    return pl.pallas_call(
        interleave_kernel,
        grid=(blocks,),
        in_specs=[pl.BlockSpec((rows, width), lambda i, f=f: (0, f(i))) for f in places],
        out_specs=pl.BlockSpec((rows, len(arrays) * width), lambda i: (0, i)),
        out_shape=jax.ShapeDtypeStruct((rows, total), arrays[0].dtype),
        cost_estimate=pl.CostEstimate(flops=rows * total, bytes_accessed=4 * rows * total, transcendentals=0),
        name="interleave",
    )(*arrays)


def separate_kernel(in_ref, out_ref):
    width = out_ref.shape[-1]
    for n in range(out_ref.shape[0]):
        out_ref[n] = in_ref[:, n * width:(n + 1) * width]


def separate(array, count, width, place=lambda i: i):
    rows, cols = array.shape
    return pl.pallas_call(
        separate_kernel,
        grid=(cols // (count * width),),
        in_specs=[pl.BlockSpec((rows, count * width), lambda i: (0, i))],
        out_specs=pl.BlockSpec((count, rows, width), lambda i: (0, 0, place(i))),
        out_shape=jax.ShapeDtypeStruct((count, rows, cols // count), array.dtype),
        cost_estimate=pl.CostEstimate(flops=rows * cols, bytes_accessed=4 * rows * cols, transcendentals=0),
        name="separate",
    )(array)


def heads_kernel(in_ref, *out_refs, span, head_dim):
    rows, cols = in_ref.shape
    heads = cols // (len(out_refs) * head_dim)
    per = span // head_dim
    for head in range(heads):
        for part, out_ref in enumerate(out_refs):
            at = (head // per * len(out_refs) + part) * span + head % per * head_dim
            out_ref[pl.ds(head, rows, stride=heads), :] = in_ref[:, at:at + head_dim]


def to_heads(array, span, head_dim):
    rows, cols = array.shape
    heads = cols // (3 * head_dim)
    step = rows // 4
    return pl.pallas_call(
        functools.partial(heads_kernel, span=span, head_dim=head_dim),
        grid=(4,),
        in_specs=[pl.BlockSpec((step, cols), lambda i: (i, 0))],
        out_specs=[pl.BlockSpec((step * heads, head_dim), lambda i: (i, 0))] * 3,
        out_shape=[jax.ShapeDtypeStruct((rows * heads, head_dim), F32)] * 3,
        cost_estimate=pl.CostEstimate(flops=rows * cols, bytes_accessed=8 * rows * cols, transcendentals=0),
        name="to_heads",
    )(array)


def wgrad_kernel(kind_ref, *refs, count, scale, blank):
    del kind_ref
    a1_refs, a2_refs, (b1_ref, b2_ref) = refs[:count], refs[count:2 * count], refs[2 * count:2 * count + 2]
    out_ref, t1, t2 = refs[2 * count + 2 + blank:]

    @pl.when(pl.program_id(1) == 0)
    def _():
        part = a1_refs[0].shape[1]
        for c in range(count):
            t1[c * part:(c + 1) * part] = a1_refs[c][...].T
            t2[c * part:(c + 1) * part] = a2_refs[c][...].T

    total = (dot_nn(t1[...], b1_ref[...]) + dot_nn(t2[...], b2_ref[...])) * scale
    out_ref[...] = total.reshape(out_ref.shape)


def wgrad(kind, acts, acts2, cots, cots2, chips, scale, spread=True, place=(None, None), into=None):
    tokens, cols = acts.shape
    width, tile, depth = 512, 1024, cols // 2
    tiles = depth // tile
    if spread:
        part = tile // chips
        share = [pl.BlockSpec((tokens, part), lambda i, j, k, c=c: (0, 2 * c + k[0])) for c in range(chips)]
    else:
        share = [pl.BlockSpec((tokens, tile), lambda i, j, k: (0, tiles * k[0] + i))]
    block = pl.BlockSpec((tokens, width), lambda i, j, k: (0, j))
    specs = share * 2 + [block, block]
    args = [acts] * len(share) + [acts2] * len(share) + [cots, cots2]
    at, aliases = 0, {}
    if into is not None:
        specs.append(pl.BlockSpec(memory_space=pl.ANY))
        args.append(into[0])
        at, aliases = into[1] // width, {len(args): 0}
    rows, total = place[0], place[1] or cots.shape[1]
    if rows is None:
        out_spec = pl.BlockSpec((tile, width), lambda i, j, k: (i, j + at))
        shape = (depth, total)
    else:
        out_spec = pl.BlockSpec((chips, tile // chips, width), lambda i, j, k: (0, 0, j + at))
        shape = (chips, rows, total)
    return pl.pallas_call(
        functools.partial(wgrad_kernel, count=len(share), scale=scale, blank=int(into is not None)),
        grid_spec=pltpu.PrefetchScalarGridSpec(
            num_scalar_prefetch=1,
            grid=(tiles, cots.shape[1] // width),
            in_specs=specs,
            out_specs=out_spec,
            scratch_shapes=[pltpu.VMEM((tile, tokens), BF16)] * 2,
        ),
        out_shape=jax.ShapeDtypeStruct(shape, F32),
        input_output_aliases=aliases,
        compiler_params=pltpu.CompilerParams(
            dimension_semantics=("arbitrary", "arbitrary"), vmem_limit_bytes=56 * 2**20),
        cost_estimate=pl.CostEstimate(
            flops=4 * tokens * depth * cots.shape[1],
            bytes_accessed=4 * cots.shape[1] * (tokens * tiles + depth), transcendentals=0),
        name="wgrad",
    )(kind, *args)


def solution(mesh):
    axis_name = mesh.axis_names[0]
    group_size = mesh.shape[axis_name]
    chips = group_size // 2
    pairs = [(d, d ^ 1) for d in range(group_size)]
    same_core = [[2 * c + core for c in range(chips)] for core in range(2)]

    def gather(local_shard):
        return lax.all_gather(local_shard, axis_name, axis=0, tiled=True)

    def local_step(x_in, grad_out, norm_attn, w_query, w_key, w_value, w_rel, bias_u, bias_w, w_attn_out, norm_mlp, w_up, w_down):
        batch_local, seq_len, width = x_in.shape
        num_heads, head_dim = w_query.shape[1], w_query.shape[2]
        hidden = num_heads * head_dim
        tokens = batch_local * seq_len
        span = hidden // group_size
        scale = 1.0 / (batch_local * group_size)
        me = lax.axis_index(axis_name)
        core = lax.rem(me, 2)

        def swap(value):
            return lax.ppermute(value, axis_name, pairs)

        def ring_place(chip):
            return chip ^ (chip >> 1)

        ring = []
        for d in range(group_size):
            to = (ring_place(d // 2) + (1 if d % 2 == 0 else chips - 1)) % chips
            ring.append((d, 2 * ring_place(to) + d % 2))
        here, turn = ring_place(lax.div(me, 2)), 1 - 2 * core

        def behind(steps):
            return ring_place(lax.rem(here - turn * steps + 2 * chips, chips))

        def pass_on(value):
            return lax.ppermute(value, axis_name, ring)

        def term(summed, steps):
            return lax.dynamic_index_in_dim(summed, behind(steps), 0, keepdims=False)

        def both_kinds(same, other):
            first, second = jnp.where(core == 0, same, other), jnp.where(core == 0, other, same)
            return jnp.stack([first, second], axis=1).reshape(group_size, *same.shape[1:])

        def share_rel(own):
            same = lax.all_to_all(jnp.broadcast_to(own[None], (chips, *own.shape)), axis_name, split_axis=0, concat_axis=0,
                                  tiled=True, axis_index_groups=same_core)
            return both_kinds(same, swap(same))

        def spread(summed):
            return lax.psum_scatter(summed, axis_name, scatter_dimension=0, axis_index_groups=same_core, tiled=True)

        def gather_halves(stacked, groups=None):
            full = lax.all_gather(stacked, axis_name, axis=1, tiled=True, axis_index_groups=groups)
            return with_layout_constraint(full, Layout(major_to_minor=(0, 1, 2)))

        def by_kind(device):
            return lax.rem(device, 2) * chips + lax.div(device, 2)

        x_f32 = x_in.reshape(tokens, width).astype(F32)
        dy = grad_out.reshape(tokens, width)
        vecs = lax.all_gather(jnp.stack([norm_attn, bias_u, bias_w, norm_mlp]), axis_name, axis=0)
        gain_attn = vecs[:, 0].reshape(width).astype(F32)
        u_full = vecs[:, 1:2].astype(F32)
        w_full = vecs[:, 2:3].astype(F32)
        gain_mlp = vecs[:, 3].reshape(width).astype(F32)

        qkv_own = interleave([z.reshape(-1, hidden) for z in (w_query, w_key, w_value)], span, group_size)
        qkv_full = gather(qkv_own)

        ff_half = w_up.shape[1] // 2
        part = ff_half // group_size
        up_own = separate(after(w_up, qkv_own), 2, part, by_kind)

        pos_table = sin_table(seq_len, width)
        rel_rows = after(w_rel, up_own).reshape(-1, hidden)
        rel_cols = lax.all_to_all(rel_rows, axis_name, split_axis=1, concat_axis=0, tiled=True)
        rel_own = dot_nn(pos_table, rel_cols).astype(BF16)
        rel_all = share_rel(rel_own)

        got = w_attn_out
        out_same = jnp.zeros((chips, *got.shape), BF16)
        out_same = lax.dynamic_update_slice(out_same, got[None], (behind(0), 0, 0))
        for step in range(chips - 1):
            got = pass_on(got)
            out_same = lax.dynamic_update_slice(out_same, got[None], (behind(step + 1), 0, 0))
        out_full = both_kinds(out_same, swap(out_same)).reshape(hidden, width)

        up_full = gather_halves(up_own)
        down_full = gather_halves(after(w_down, up_own).reshape(2, part, width), [same_core[0] + same_core[1]])

        h_attn = rms_norm(x_f32, gain_attn)
        shape3 = (batch_local, seq_len, -1)
        qkv = dot_nn(h_attn, qkv_full).astype(BF16).reshape(shape3)
        context = attn_fwd(qkv, rel_all, u_full, w_full, head_dim).reshape(tokens, hidden)
        x1_f32 = (x_f32 + dot_nn(context, out_full)).astype(BF16).astype(F32)
        h_mlp = rms_norm(x1_f32, gain_mlp)

        def feed(acts, weight):
            pre = dot_nn(acts, weight).astype(BF16)
            return pre, gelu_tanh(pre.astype(F32)).astype(BF16)

        def unfeed(cots, weight, pre):
            d_act = dot_nt(cots, weight).astype(BF16)
            return (d_act.astype(F32) * gelu_slope(pre.astype(F32))).astype(BF16)

        kind = core[None]
        dy_theirs = swap(after(dy, h_attn))
        attn_theirs = swap(h_attn)
        context_theirs = swap(context)

        pre0, act0 = feed(h_mlp, up_full[0])
        act0_theirs = swap(act0)
        pre1, act1 = feed(after(h_mlp, act0), up_full[1])
        sum_down0 = wgrad(kind, after(act0, act1), act0_theirs, dy, dy_theirs, chips, scale, False)
        act1_theirs = swap(act1)
        d_pre0 = unfeed(after(dy, sum_down0), down_full[0], pre0)
        d_pre0_theirs = swap(d_pre0)
        hidden_theirs = swap(h_mlp)
        sum_down1 = wgrad(kind, after(act1, d_pre0), act1_theirs, dy, dy_theirs, chips, scale, False)
        d_pre1 = unfeed(after(dy, sum_down1), down_full[1], pre1)
        d_pre1_theirs = swap(d_pre1)
        both = (None, 2 * ff_half)
        sum_up = wgrad(kind, h_mlp, hidden_theirs, after(d_pre0, d_pre1), d_pre0_theirs, chips, scale,
                       place=both)
        sum_up = wgrad(kind, h_mlp, hidden_theirs, d_pre1, d_pre1_theirs, chips, scale,
                       place=both, into=(sum_up, ff_half))
        d_h_part = dot_nt(after(d_pre0, sum_up), up_full[0])
        d_h_mlp = (d_h_part + dot_nt(after(d_pre1, d_h_part), up_full[1])).astype(BF16)
        grad_down = jnp.concatenate([spread(sum_down0), spread(sum_down1)], axis=0)
        grad_up = spread(sum_up)

        d_x1_norm, grad_norm_mlp = jax.vjp(rms_norm, x1_f32, gain_mlp)[1](d_h_mlp)
        d_x1 = (dy.astype(F32) + d_x1_norm).astype(BF16)
        d_x1_theirs = swap(d_x1)
        d_context = dot_nt(d_x1, out_full).astype(BF16).reshape(shape3)
        d_qkv, d_rel, d_u, d_w = attn_bwd(
            qkv, rel_all, u_full, w_full, d_context, head_dim, 0, group_size)
        d_qkv = d_qkv.reshape(tokens, -1)
        d_qkv_theirs = swap(d_qkv)
        d_rel = d_rel.reshape(chips, 2, seq_len, span)
        got_rel = swap(lax.dynamic_index_in_dim(d_rel, 1 - core, 1, keepdims=False))
        sum_o = wgrad(kind, context, context_theirs, after(d_x1, d_qkv), d_x1_theirs, chips, scale)
        sum_o = sum_o.reshape(chips, -1, width)
        sum_rel = lax.dynamic_index_in_dim(d_rel, core, 1, keepdims=False) + got_rel
        part_o, part_rel = term(sum_o, 1), term(sum_rel, 1)
        got_o, got_rel = pass_on(part_o), pass_on(part_rel)
        sum_qkv = wgrad(kind, h_attn, attn_theirs, after(d_qkv, part_o, part_rel), d_qkv_theirs, chips, scale)
        grad_qkv = spread(sum_qkv)
        part_o, part_rel = term(after(sum_o, sum_qkv), 2) + got_o, term(after(sum_rel, sum_qkv), 2) + got_rel
        got_o, got_rel = pass_on(part_o), pass_on(part_rel)
        y_out = (x1_f32 + dot_nn(after(act0, part_o, part_rel), down_full[0]) + dot_nn(act1, down_full[1])).astype(BF16)
        part_o, part_rel = term(after(sum_o, y_out), 3) + got_o, term(after(sum_rel, y_out), 3) + got_rel
        got_o, got_rel = pass_on(part_o), pass_on(part_rel)
        d_h_attn = dot_nt(after(d_qkv, part_o, part_rel), qkv_full).astype(BF16)
        d_x_norm, grad_norm_attn = jax.vjp(rms_norm, x_f32, gain_attn)[1](d_h_attn)
        grad_attn_out = term(after(sum_o, d_h_attn), 0) + got_o
        d_rel_own = (term(after(sum_rel, d_h_attn), 0) + got_rel).reshape(seq_len // BLK, BLK, span)
        d_rel_own = jnp.flip(d_rel_own, axis=1).reshape(seq_len, span).astype(BF16)
        d_rel_all = share_rel(d_rel_own)
        grad_x = (d_x1.astype(F32) + d_x_norm).astype(BF16)

        table_own = lax.dynamic_slice(pos_table, (0, me * (width // group_size)), (seq_len, width // group_size))
        grad_rel = dot_tn(table_own, d_rel_all.transpose(1, 0, 2).reshape(seq_len, hidden)) * scale
        grad_up = interleave([grad_up, grad_up], part, group_size, [by_kind, lambda d: by_kind(d) + group_size])
        grad_query, grad_key, grad_value = to_heads(grad_qkv, span, head_dim)

        small = jnp.stack([grad_norm_attn.reshape(group_size, span), jnp.sum(d_u, axis=1), jnp.sum(d_w, axis=1),
                           grad_norm_mlp.reshape(group_size, span)], axis=1)
        small = lax.psum_scatter(small * scale, axis_name, scatter_dimension=0, tiled=True)[0]

        heads3 = (-1, num_heads, head_dim)
        return (y_out.reshape(x_in.shape), grad_x.reshape(x_in.shape), small[0], grad_query.reshape(heads3),
                grad_key.reshape(heads3), grad_value.reshape(heads3), grad_rel.reshape(heads3), small[1], small[2],
                grad_attn_out, small[3], grad_up, grad_down)

    sharded = P(axis_name)
    return jax.shard_map(local_step, mesh=mesh, in_specs=(sharded,) * 13, out_specs=(sharded,) * 13, check_vma=False)
```
